512 devices in a mesh: ax: 16 (over y, core), th: 16 (over x_hi, z), grp: 2 (over x_lo).
Axes of the slice: x: 4 (x_hi: 2, x_lo: 2; x = x_hi * 2 + x_lo), y: 8, z: 8, core: 2. Of those that a mesh axis runs over, the one named last changes fastest.
Arguments:
- fields: float32 [4, 512, 384, 128], P(None, ('ax', 'grp'), 'th'), may hold values from -5 to 5, as said below
- wall_temp: float32 [512, 384, 64], P(('ax', 'grp'), 'th'), may hold values from -5 to 5
- fluid_metric: float32 [128], replicated, may hold values from 0.5 to 2
- fluid_radial_inverses: float32 [2, 128, 128], replicated, may hold values from 0 to 1, as said below
- wall_metric: float32 [64], replicated, may hold values from 0.5 to 2
- wall_inverse: float32 [64, 64], replicated, may hold values from 0 to 1, as said below
Outputs:
- predicted_coolant_state: float32 [4, 512, 384, 128], P(None, ('ax', 'grp'), 'th')
- new_wall: float32 [512, 384, 64], P(('ax', 'grp'), 'th')
The draws below stay inside these ranges and needn't reach their ends.
Inputs may be any that keep to these rules, and one draw needn't show every extreme that they name: `fields`: components in the order axial, circumferential, radial velocity, temperature. fluid_radial_inverses[0] and fluid_radial_inverses[1] are the inverses of I - 0.4 L and I - 0.6 L with (L v)_j = m_j (e_j (v_(j+1) - v_j) - e_(j-1) (v_j - v_(j-1))), m = fluid_metric, e_j = (m_j + m_(j+1)) / 2 for j < 127, e_(127) = m_(127), e_(-1) = 0 and v_128 = 0. wall_inverse is the inverse of I - 0.8 L with L built as for the fluid from m = wall_metric, but e_(-1) = m_0, v_(-1) = 0 and e_(63) = 0.
All inputs are finite; a program needn't handle non-finite values.
Results may differ from the reference program's by a relative error of at most 0.00035.
Values sent between devices are 32-bit elements; how exact they have to be, the bound alone decides.
A program may use at most 64 MiB of HBM per device.

```python
import math
import jax
import jax.numpy as jnp
from jax import lax

X = 512
THETA = 384
R = 128
RW = 64


VISCOUS = 0.4


CONDUCT_T = 0.6


CONDUCT_W = 0.8


def radial_inverse(metric, inner_edge, outer_edge, factor):
    count = metric.shape[0]
    between = 0.5 * (metric[:-1] + metric[1:])
    upper_edges = jnp.concatenate([between, outer_edge])
    before = jnp.concatenate([inner_edge, between])
    diagonal = -metric * (upper_edges + before)
    operator = jnp.diag(diagonal) + jnp.diag(metric[:-1] * between, 1) + jnp.diag(metric[1:] * between, -1)
    matrix = jnp.eye(count, dtype=jnp.float32) - factor * operator
    return jnp.linalg.solve(matrix, jnp.eye(count, dtype=jnp.float32))


def draw_metric(key, count):
    sample = jax.random.uniform(key, (count,), jnp.float32, math.log(0.5), math.log(2.0))
    return jnp.clip(jnp.exp(sample), 0.5, 2.0)


def fluid_grid(key):
    metric = draw_metric(jax.random.fold_in(key, 11), R)
    inner_edge = jnp.zeros((1,), jnp.float32)
    outer_edge = metric[-1:]
    coolant_speed_vector = radial_inverse(metric, inner_edge, outer_edge, VISCOUS)
    heat = radial_inverse(metric, inner_edge, outer_edge, CONDUCT_T)
    return (metric, jnp.stack([coolant_speed_vector, heat]))


def wall_grid(key):
    metric = draw_metric(jax.random.fold_in(key, 12), RW)
    inner_edge = metric[:1]
    outer_edge = jnp.zeros((1,), jnp.float32)
    return (metric, radial_inverse(metric, inner_edge, outer_edge, CONDUCT_W))


def draw_fields(key, part):
    sample = jax.random.truncated_normal(jax.random.fold_in(key, 3), -5.0, 5.0, (4, X, THETA, R), jnp.float32)
    return sample


def draw_fluid_metric(key, part):
    return fluid_grid(key)[0]


def draw_fluid_radial_inverses(key, part):
    return fluid_grid(key)[1]


def draw_wall_metric(key, part):
    return wall_grid(key)[0]


def draw_wall_inverse(key, part):
    return wall_grid(key)[1]


def steps_of(own_key, shape, shards, smallest, high):
    loudness, own = 1.0, jax.random.fold_in(own_key, 6)
    for position, parts in shards:
        heights = jnp.exp(jax.random.uniform(jax.random.fold_in(own, position), (parts,), jnp.float32, smallest / len(shards), high / len(shards)))
        loudness = loudness * jnp.repeat(heights, shape[position] // parts).reshape([-1 if axis == position else 1 for axis in range(len(shape))])
    return loudness


def normal_values(rng, dims, scale, reach, split=(), kind=jnp.bfloat16):
    loudness = steps_of(rng, dims, split, -0.22, 0.18) if split else 1.0
    array = jax.random.normal(rng, dims, jnp.float32) * scale * loudness
    return jnp.minimum(jnp.maximum(array, -reach), reach).astype(kind)


def setup_inputs(seed: int = 0) -> dict:
    keys = jax.random.split(jax.random.key(seed), 7)
    return {
        "fields": draw_fields(jax.random.fold_in(keys[6], 71), 0),
        "wall_temp": normal_values(keys[1], (X, THETA, RW), 1.0, 5.0, ((0, 32), (1, 16)), jnp.float32),
        "fluid_metric": draw_fluid_metric(jax.random.fold_in(keys[6], 71), 0),
        "fluid_radial_inverses": draw_fluid_radial_inverses(jax.random.fold_in(keys[6], 71), 0),
        "wall_metric": draw_wall_metric(jax.random.fold_in(keys[6], 71), 0),
        "wall_inverse": draw_wall_inverse(jax.random.fold_in(keys[6], 71), 0),
    }


EXACT_PRECISION = lax.Precision.HIGHEST
ADVECT_X = 0.08
ADVECT_T = 0.08
ADVECT_R = 0.15
LATERAL_U = 0.03
LATERAL_T = 0.04
LATERAL_W = 0.1
COUPLE_T = 0.6
COUPLE_W = 0.8

def tables(points):
    positions = jnp.arange(points)
    offset = positions[:, None] - positions[None, :]
    spacing = 2.0 * math.pi / points
    parity = (1 - 2 * (offset % 2)).astype(jnp.float32)
    nonzero = offset != 0
    polar_azimuths = jnp.where(nonzero, offset.astype(jnp.float32) * (0.5 * spacing), 1.0)
    first_table = jnp.where(nonzero, 0.5 * spacing * parity / jnp.tan(polar_azimuths), 0.0)
    second = jnp.where(nonzero, -parity * spacing * spacing / (2.0 * jnp.sin(polar_azimuths) ** 2), -(math.pi ** 2 / 3.0 + spacing * spacing / 6.0))
    return jnp.concatenate([first_table, second], axis=0).astype(jnp.float32)

def fluid_radius(metric):
    spread = 1.0 / metric
    spread_total = jnp.sum(spread)
    beyond = jnp.cumsum(spread[::-1])[::-1]
    return 1.0 - 0.5 * (beyond - 0.5 * spread) / spread_total

def shell_distance_centre(metric):
    spread = 1.0 / metric
    spread_total = jnp.sum(spread)
    return 1.0 + 0.2 * (jnp.cumsum(spread) - 0.5 * spread) / spread_total

def reference(fields, wall_temp, fluid_metric, fluid_radial_inverses, wall_metric, wall_inverse):
    axial_lookup_table = tables(X)
    circle_table = tables(THETA)
    radius = fluid_radius(fluid_metric)
    wall_rad = shell_distance_centre(wall_metric)
    ghost_wall = wall_temp[:, :, 0]
    fluid_last = fields[3, :, :, -1]
    results = []
    for field_index in range(4):
        current = fields[field_index]
        lateral = LATERAL_T if field_index == 3 else LATERAL_U
        axial_derived = jnp.einsum('ij,jtr->itr', axial_lookup_table, current, precision=EXACT_PRECISION)
        axial_terms = -ADVECT_X * fields[0] * axial_derived[:X] + lateral * axial_derived[X:]
        circle_derived = jnp.einsum('ij,xjr->xir', circle_table, current, precision=EXACT_PRECISION)
        circle_terms = (-ADVECT_T * fields[1] * circle_derived[:, :THETA] + lateral * circle_derived[:, THETA:] / radius) / radius
        if field_index == 3:
            ghost = ghost_wall
        else:
            ghost = jnp.zeros_like(ghost_wall)
        upper_cells = jnp.concatenate([current[:, :, 1:], ghost[:, :, None]], axis=2)
        lower_cells = jnp.concatenate([current[:, :, :1], current[:, :, :-1]], axis=2)
        radial_terms = -ADVECT_R * fields[2] * fluid_metric * (upper_cells - lower_cells) * 0.5
        right_side = current + axial_terms + circle_terms + radial_terms
        if field_index == 3:
            last_cell = jnp.arange(R) == R - 1
            fluid_lift = COUPLE_T * fluid_metric[-1] * fluid_metric[-1] * ghost_wall
            right_side = right_side + jnp.where(last_cell, fluid_lift[:, :, None], 0.0)
            inverse = fluid_radial_inverses[1]
        else:
            inverse = fluid_radial_inverses[0]
        results.append(jnp.einsum('by,ldy->ldb', inverse, right_side, precision=EXACT_PRECISION))
    predicted_coolant_state = jnp.stack(results)
    wall_axial = jnp.einsum('ij,jtr->itr', axial_lookup_table, wall_temp, precision=EXACT_PRECISION)
    wall_circle = jnp.einsum('ij,xjr->xir', circle_table, wall_temp, precision=EXACT_PRECISION)
    first_cell = jnp.arange(RW) == 0
    wall_lift = COUPLE_W * wall_metric[0] * wall_metric[0] * fluid_last
    wall_side = wall_temp + LATERAL_W * wall_axial[X:] + LATERAL_W * wall_circle[:, THETA:] / (wall_rad * wall_rad) + jnp.where(first_cell, wall_lift[:, :, None], 0.0)
    new_wall = jnp.einsum('by,ldy->ldb', wall_inverse, wall_side, precision=EXACT_PRECISION)
    return (predicted_coolant_state, new_wall)
```

```python
import functools

import jax
import jax.numpy as jnp
import numpy as np
from jax import lax
from jax.experimental import pallas as pl
from jax.experimental.pallas import tpu as pltpu
from jax.sharding import PartitionSpec as P

MESH = pl.DeviceIdType.MESH
F32 = jnp.float32
BF16 = jnp.bfloat16

X = 512
THETA = 384
R = 128
RW = 64
XL = 16
TL = 24
NT = 16
NA = 32

ADVECT_X = 0.08
ADVECT_T = 0.08
ADVECT_R = 0.15
LATERAL_U = 0.03
LATERAL_T = 0.04
LATERAL_W = 0.1
COUPLE_T = 0.6
COUPLE_W = 0.8


def folded_tables(points):
    spacing = 2.0 * np.pi / points
    offset = np.arange(points)[:, None] - np.arange(points)[None, :]
    parity = 1.0 - 2.0 * (offset % 2)
    angle = np.where(offset != 0, offset * 0.5 * spacing, 1.0)
    first = np.where(offset != 0, 0.5 * spacing * parity / np.tan(angle), 0.0)
    second = np.where(
        offset != 0,
        -parity * spacing**2 / (2.0 * np.sin(angle) ** 2),
        -(np.pi**2 / 3.0 + spacing**2 / 6.0),
    )
    half = points // 2
    parts = []
    for sign in (1.0, -1.0):
        both = np.concatenate(
            [0.5 * (table[:half, :half] + sign * table[:half, half:]) for table in (first, second)], axis=0
        ).astype(np.float32)
        high = both.astype(BF16)
        low = (both - high.astype(np.float32)).astype(BF16)
        parts.append(np.stack([high, low]))
    return np.stack(parts)


def split(value):
    high = value.astype(BF16)
    low = (value - high.astype(F32)).astype(BF16)
    return high, low


def dot(a, b):
    return jnp.dot(a, b, preferred_element_type=F32)


def dot_t(a, b):
    return lax.dot_general(a, b, (((1,), (1,)), ((), ())), preferred_element_type=F32)


def apply_folded(table, rows, top, bottom):
    results = []
    for which, value in ((0, top + bottom), (1, top - bottom)):
        high, low = split(value)
        t_high = table[which, 0, rows, :]
        t_low = table[which, 1, rows, :]
        results.append(dot(t_high, high) + dot(t_high, low) + dot(t_low, high))
    return results[0] + results[1], results[0] - results[1]


def kernel(
    fields_h, wall_h, fm, inv, wm, winv, ttab_h, xtab_h,
    out_h, wout_h,
    F, W, ttab, xtab,
    fT, WP, wT,
    Qt, Qx, Wt, Wx,
    Rt, Rx, WRt, WRx, Wn,
    cih, axh, cwh, awh,
    base, wbase, obuf, wobuf,
    ld, st,
    sT, rT, sX, rX, sWT, rWT, sWX, rWX,
    bsT, brT, bsX, brX, bsWT, brWT, bsWX, brWX,
):
    ax = lax.axis_index("ax")
    th = lax.axis_index("th")
    grp = lax.axis_index("grp")
    a = ax * 2 + grp
    y = lax.div(ax, 2)
    core = lax.rem(ax, 2)
    xh = lax.div(th, 8)
    z = lax.rem(th, 8)
    odd_y = lax.rem(y, 2)
    x_wall = jnp.logical_and(core == 0, grp == odd_y)
    x_fluid = jnp.logical_not(x_wall)
    my_theta = 3 * y + core * (1 + grp)
    t_wall = xh == lax.rem(z, 2)

    barrier = pltpu.get_barrier_semaphore()

    def greet_t(k, _):
        pl.semaphore_signal(barrier, inc=1, device_id=(ax, lax.rem(th + k, NT), grp), device_id_type=MESH)
        return 0

    def greet_a(k, _):
        peer = lax.rem(a + k, NA)
        pl.semaphore_signal(
            barrier, inc=1, device_id=(lax.div(peer, 2), th, lax.rem(peer, 2)), device_id_type=MESH
        )
        return 0

    lax.fori_loop(1, NT, greet_t, 0)
    lax.fori_loop(1, NA, greet_a, 0)

    load_f = pltpu.make_async_copy(fields_h, F, ld.at[0])
    load_w = pltpu.make_async_copy(wall_h, W, ld.at[1])
    load_t = pltpu.make_async_copy(ttab_h, ttab, ld.at[2])
    load_x = pltpu.make_async_copy(xtab_h, xtab, ld.at[3])
    load_f.start()
    load_w.start()
    load_t.start()
    load_x.start()
    load_f.wait()

    F2 = F.reshape(4 * XL * TL, R)

    def turn(t, _):
        for c in range(4):
            fT[c // 2, t, c % 2] = F2[pl.ds(c * XL * TL + t, XL, stride=TL), :]
        return 0

    lax.fori_loop(0, TL, turn, 0)
    load_w.wait()
    for p in range(8):
        WP[p] = jnp.concatenate([W[p], W[p + 8]], axis=1)
    WP2 = WP.reshape(8 * TL, R)
    for t in range(TL):
        wT[t] = WP2[pl.ds(t, 8, stride=TL), :]

    pl.semaphore_wait(barrier, NT - 1 + NA - 1)

    def offset(i):
        return 4 + lax.div(i + 1, 2) * (1 - 2 * lax.rem(i, 2))

    def send(remote, src, dst, s_sem, r_sem, device):
        @pl.when(remote)
        def _():
            pltpu.make_async_remote_copy(
                src_ref=src, dst_ref=dst, send_sem=s_sem, recv_sem=r_sem, device_id=device, device_id_type=MESH
            ).start()

        @pl.when(jnp.logical_not(remote))
        def _():
            pltpu.make_async_copy(src, dst, r_sem).start()

    def theta_peer(i, flip):
        return lax.rem(xh + flip, 2) * 8 + lax.rem(z + offset(i), 8)

    def send_chunk(ch):
        def step(i, _):
            for flip in (1, 0):
                t = theta_peer(i, flip)
                send(
                    t != th, F.at[pl.ds(2 * ch, 2), t], Qt.at[pl.ds(2 * ch, 2), pl.ds(TL * th, TL)],
                    sT.at[ch], rT.at[ch], (ax, t, grp),
                )
            yy = lax.rem(y + offset(i), 8)
            for k in range(3):
                theta = 3 * yy + k
                c_to = (k + 1) // 2
                g_to = k // 2 + (1 - c_to) * (1 - lax.rem(yy, 2))
                a_to = 4 * yy + 2 * c_to + g_to
                send(
                    a_to != a, fT.at[ch, theta], Qx.at[pl.ds(2 * ch, 2), pl.ds(XL * a, XL)],
                    sX.at[ch], rX.at[ch], (2 * yy + c_to, th, g_to),
                )
            return 0

        lax.fori_loop(0, 8, step, 0)

    def send_wall():
        def step(i, _):
            p = lax.rem(z + offset(i), 8)
            t = lax.rem(p, 2) * 8 + p
            send(t != th, WP.at[p], Wt.at[pl.ds(TL * th, TL)], sWT, rWT, (ax, t, grp))
            yy = lax.rem(y + offset(i), 8)
            a_to = 4 * yy + lax.rem(yy, 2)
            send(
                a_to != a, wT.at[pl.ds(3 * yy, 3)], Wx.at[:, pl.ds(8 * a, 8)],
                sWX, rWX, (2 * yy, th, lax.rem(yy, 2)),
            )
            return 0

        lax.fori_loop(0, 8, step, 0)

    send_chunk(0)
    send_wall()
    send_chunk(1)

    lane = lax.broadcasted_iota(jnp.int32, (TL, R), 1)
    m = fm[...]
    row_r = -0.5 * ADVECT_R * m
    row_lift = COUPLE_T * m * m
    wm2 = jnp.concatenate([wm[...], wm[...]], axis=1)
    row_wlift = COUPLE_W * wm2 * wm2

    kk = lax.broadcasted_iota(jnp.int32, (R, R), 0)
    jj = lax.broadcasted_iota(jnp.int32, (R, R), 1)
    spread = 1.0 / m
    spread_t = jnp.broadcast_to(spread, (R, R)).T
    beyond = jnp.sum(jnp.where(kk >= jj, spread_t, 0.0), axis=0, keepdims=True)
    total = jnp.sum(spread_t, axis=0, keepdims=True)
    radius = 1.0 - 0.5 * (beyond - 0.5 * spread) / total
    row_t1 = -ADVECT_T / radius
    row_t2 = 1.0 / (radius * radius)
    wspread = 1.0 / wm2
    wspread_t = jnp.broadcast_to(wspread, (R, R)).T
    within = jnp.sum(jnp.where(kk <= lax.rem(jj, RW), wspread_t, 0.0), axis=0, keepdims=True)
    wtotal = jnp.sum(jnp.where(kk < RW, wspread_t, 0.0), axis=0, keepdims=True)
    wradius = 1.0 + 0.2 * (within - 0.5 * wspread) / wtotal
    row_w2 = LATERAL_W / (wradius * wradius)

    def prepare(p, _):
        pair = WP[p]
        for h in range(2):
            x = p + 8 * h
            u_r = F[2, x] * row_r
            ghost = pltpu.roll(pair, 127 - 64 * h, axis=1)
            for c in range(4):
                q = F[c, x]
                edge = ghost if c == 3 else 0.0
                upper = jnp.where(lane == R - 1, edge, pltpu.roll(q, R - 1, axis=1))
                lower = jnp.where(lane == 0, q, pltpu.roll(q, 1, axis=1))
                value = q + u_r * (upper - lower)
                if c == 3:
                    value = value + jnp.where(lane == R - 1, row_lift * ghost, 0.0)
                base[c, x] = value
        last_0 = pltpu.roll(F[3, p], 1, axis=1)
        last_1 = pltpu.roll(F[3, p + 8], 65, axis=1)
        wbase[p] = pair + jnp.where(
            lane == 0, row_wlift * last_0, jnp.where(lane == RW, row_wlift * last_1, 0.0)
        )
        return 0

    lax.fori_loop(0, 8, prepare, 0)
    load_t.wait()
    load_x.wait()

    def full(ref, sem):
        pltpu.make_async_copy(ref, ref, sem).wait()

    half_t = THETA // 2
    half_x = X // 2

    def lam(ch, cc):
        return jnp.where(ch == 1, LATERAL_T, LATERAL_U) if cc == 1 else LATERAL_U

    def theta_chunk(ch):
        both = pl.ds(2 * ch, 2)
        full(Qt.at[both], rT.at[ch])
        top = jnp.concatenate([Qt[2 * ch, :half_t], Qt[2 * ch + 1, :half_t]], axis=1)
        bottom = jnp.concatenate([Qt[2 * ch, half_t:], Qt[2 * ch + 1, half_t:]], axis=1)
        firsts = apply_folded(ttab, slice(0, half_t), top, bottom)
        seconds = apply_folded(ttab, slice(half_t, THETA), top, bottom)
        for h in range(2):
            rows = slice(h * half_t, (h + 1) * half_t)
            swirl = Qt[1, rows] * row_t1
            for cc in range(2):
                cols = slice(cc * R, (cc + 1) * R)
                Rt[2 * ch + cc, rows] = swirl * firsts[h][:, cols] + seconds[h][:, cols] * (row_t2 * lam(ch, cc))

        def step(i, _):
            for flip in (1, 0):
                t = theta_peer(i, flip)
                send(
                    t != th, Rt.at[both, pl.ds(TL * t, TL)], cih.at[both, th], bsT.at[ch], brT.at[ch], (ax, t, grp)
                )
            return 0

        lax.fori_loop(0, 8, step, 0)

    def axial_chunk(ch):
        both = pl.ds(2 * ch, 2)
        full(Qx.at[both], rX.at[ch])
        top = jnp.concatenate([Qx[2 * ch, :half_x], Qx[2 * ch + 1, :half_x]], axis=1)
        bottom = jnp.concatenate([Qx[2 * ch, half_x:], Qx[2 * ch + 1, half_x:]], axis=1)
        firsts = apply_folded(xtab, slice(0, half_x), top, bottom)
        seconds = apply_folded(xtab, slice(half_x, X), top, bottom)
        for h in range(2):
            rows = slice(h * half_x, (h + 1) * half_x)
            stream = Qx[0, rows] * (-ADVECT_X)
            for cc in range(2):
                cols = slice(cc * R, (cc + 1) * R)
                Rx[2 * ch + cc, rows] = stream * firsts[h][:, cols] + seconds[h][:, cols] * lam(ch, cc)

        def step(i, _):
            yy = lax.rem(y + offset(i), 8)
            for k in range(4):
                a_to = 4 * yy + k
                send(
                    a_to != a, Rx.at[both, pl.ds(XL * a_to, XL)], axh.at[ch, my_theta],
                    bsX.at[ch], brX.at[ch], (2 * yy + k // 2, th, k % 2),
                )
            return 0

        lax.fori_loop(0, 8, step, 0)

    def theta_wall():
        full(Wt, rWT)
        seconds = apply_folded(ttab, slice(half_t, THETA), Wt[:half_t], Wt[half_t:])
        for h in range(2):
            WRt[h * half_t:(h + 1) * half_t] = seconds[h] * row_w2

        def step(i, _):
            for flip in (1, 0):
                t = theta_peer(i, flip)
                send(t != th, WRt.at[pl.ds(TL * t, TL)], cwh.at[z], bsWT, brWT, (ax, t, grp))
            return 0

        lax.fori_loop(0, 8, step, 0)

    low8 = lax.broadcasted_iota(jnp.int32, (8, R), 1) < RW

    def axial_wall():
        full(Wx, rWX)

        def unpack(s, _):
            rows = pl.ds(pl.multiple_of(8 * s, 8), 8)
            w0, w1, w2 = Wx[0, rows], Wx[1, rows], Wx[2, rows]
            even = pl.ds(pl.multiple_of(16 * s, 8), 8)
            odd = pl.ds(pl.multiple_of(16 * s + 8, 8), 8)
            Wn[even, 0:R] = jnp.where(low8, w0, pltpu.roll(w1, RW, axis=1))
            Wn[odd, 0:R] = jnp.where(low8, pltpu.roll(w0, RW, axis=1), w1)
            Wn[even, R:2 * R] = w2
            Wn[odd, R:2 * R] = pltpu.roll(w2, RW, axis=1)
            return 0

        lax.fori_loop(0, NA, unpack, 0)
        seconds = apply_folded(xtab, slice(half_x, X), Wn[:half_x], Wn[half_x:])
        for h in range(2):
            Wn[h * half_x:(h + 1) * half_x] = seconds[h] * LATERAL_W

        def pack(s, _):
            rows = pl.ds(pl.multiple_of(8 * s, 8), 8)
            even = pl.ds(pl.multiple_of(16 * s, 8), 8)
            odd = pl.ds(pl.multiple_of(16 * s + 8, 8), 8)
            e01, o01 = Wn[even, 0:R], Wn[odd, 0:R]
            WRx[0, rows] = jnp.where(low8, e01, pltpu.roll(o01, RW, axis=1))
            WRx[1, rows] = jnp.where(low8, pltpu.roll(e01, RW, axis=1), o01)
            WRx[2, rows] = jnp.where(low8, Wn[even, R:2 * R], pltpu.roll(Wn[odd, R:2 * R], RW, axis=1))
            return 0

        lax.fori_loop(0, NA, pack, 0)

        def step(i, _):
            yy = lax.rem(y + offset(i), 8)
            for k in range(4):
                a_to = 4 * yy + k
                send(
                    a_to != a, WRx.at[:, pl.ds(8 * a_to, 8)], awh.at[pl.ds(3 * y, 3)],
                    bsWX, brWX, (2 * yy + k // 2, th, k % 2),
                )
            return 0

        lax.fori_loop(0, 8, step, 0)

    theta_chunk(0)
    pl.when(x_fluid)(lambda: axial_chunk(0))
    pl.when(x_wall)(axial_wall)
    pl.when(t_wall)(theta_wall)
    theta_chunk(1)
    pl.when(x_fluid)(lambda: axial_chunk(1))

    axh2 = axh.reshape(4 * XL * TL, R)

    def inverse_parts(matrix):
        high, low = split(matrix)
        return jnp.concatenate([high, high, low], axis=1)

    def value_parts(value):
        high, low = split(value)
        return jnp.concatenate([high, low, high], axis=1)

    def finish(ch):
        full(cih.at[pl.ds(2 * ch, 2)], brT.at[ch])
        full(axh.at[ch], brX.at[ch])
        for cc in range(2):
            c = 2 * ch + cc

            def gather(x, _):
                axial = axh2[pl.ds(ch * 2 * XL * TL + cc * XL + x, TL, stride=2 * XL), :]
                base[c, x] = base[c, x] + cih[c, x] + axial
                return 0

            lax.fori_loop(0, XL, gather, 0)
            matrix = inverse_parts(inv[1 if c == 3 else 0])
            value = value_parts(base[c].reshape(XL * TL, R))
            obuf[c] = dot_t(value, matrix).reshape(XL, TL, R)
            pltpu.make_async_copy(obuf.at[c], out_h.at[c], st.at[c]).start()

    finish(0)
    full(cwh, brWT)
    full(awh, brWX)
    awh2 = awh.reshape(8 * TL, R)

    def gather_wall(p, _):
        wbase[p] = wbase[p] + cwh[p] + awh2[pl.ds(p, TL, stride=8), :]
        return 0

    lax.fori_loop(0, 8, gather_wall, 0)
    value = value_parts(wbase[...].reshape(8 * TL, R))
    nothing = jnp.zeros((RW, RW), F32)
    for h in range(2):
        pair = [winv[...], nothing] if h == 0 else [nothing, winv[...]]
        matrix = inverse_parts(jnp.concatenate(pair, axis=1))
        wobuf[8 * h:8 * h + 8] = dot_t(value, matrix).reshape(8, TL, RW)
    pltpu.make_async_copy(wobuf, wout_h, st.at[4]).start()
    finish(1)

    for ch in range(2):
        full(F.at[pl.ds(0, 2), pl.ds(0, NT - 1)], sT.at[ch])
        full(F.at[pl.ds(0, 2), pl.ds(0, NT - 1)], bsT.at[ch])

        @pl.when(x_fluid)
        def _():
            full(fT.at[ch, pl.ds(0, TL - 1)], sX.at[ch])
            full(Rx.at[pl.ds(0, 2), pl.ds(0, X - XL)], bsX.at[ch])

        @pl.when(x_wall)
        def _():
            full(fT.at[ch], sX.at[ch])

    @pl.when(t_wall)
    def _():
        full(WP.at[pl.ds(0, 7)], sWT)
        full(WRt.at[pl.ds(0, THETA - TL)], bsWT)

    @pl.when(jnp.logical_not(t_wall))
    def _():
        full(WP, sWT)

    @pl.when(x_wall)
    def _():
        full(wT.at[pl.ds(0, TL - 3)], sWX)
        full(WRx.at[:, pl.ds(0, 8 * (NA - 1))], bsWX)

    @pl.when(x_fluid)
    def _():
        full(wT, sWX)

    for c in range(4):
        pltpu.make_async_copy(obuf.at[c], out_h.at[c], st.at[c]).wait()
    pltpu.make_async_copy(wobuf, wout_h, st.at[4]).wait()


def shards(fields, wall_temp, fluid_metric, fluid_radial_inverses, wall_metric, wall_inverse):
    vmem = pl.BlockSpec(memory_space=pltpu.VMEM)
    hbm = pl.BlockSpec(memory_space=pl.ANY)
    dma = pltpu.SemaphoreType.DMA
    ttab = jnp.asarray(folded_tables(THETA))
    xtab = jnp.asarray(folded_tables(X))

    def buf(*shape, dtype=F32):
        return pltpu.VMEM(shape, dtype)

    return pl.pallas_call(
        kernel,
        out_shape=(
            jax.ShapeDtypeStruct((4, XL, TL, R), F32),
            jax.ShapeDtypeStruct((XL, TL, RW), F32),
        ),
        in_specs=[hbm, hbm, vmem, vmem, vmem, vmem, hbm, hbm],
        out_specs=(hbm, hbm),
        scratch_shapes=[
            buf(4, XL, TL, R), buf(XL, TL, RW), buf(*ttab.shape, dtype=BF16), buf(*xtab.shape, dtype=BF16),
            buf(2, TL, 2, XL, R), buf(8, TL, R), buf(TL, 8, R),
            buf(4, THETA, R), buf(4, X, R), buf(THETA, R), buf(3, X // 2, R),
            buf(4, THETA, R), buf(4, X, R), buf(THETA, R), buf(3, X // 2, R), buf(X, 2 * R),
            buf(4, XL, TL, R), buf(2, TL, 2, XL, R), buf(8, TL, R), buf(TL, 8, R),
            buf(4, XL, TL, R), buf(8, TL, R), buf(4, XL, TL, R), buf(XL, TL, RW),
            dma((4,)), dma((5,)),
            dma((2,)), dma((2,)), dma((2,)), dma((2,)), dma, dma, dma, dma,
            dma((2,)), dma((2,)), dma((2,)), dma((2,)), dma, dma, dma, dma,
        ],
        compiler_params=pltpu.CompilerParams(collective_id=0, has_side_effects=True),
    )(
        fields, wall_temp, fluid_metric.reshape(1, R), fluid_radial_inverses,
        wall_metric.reshape(1, RW), wall_inverse, ttab, xtab,
    )


def solution(mesh):
    in_specs = (
        P(None, ("ax", "grp"), "th", None),
        P(("ax", "grp"), "th", None),
        P(),
        P(),
        P(),
        P(),
    )
    out_specs = (P(None, ("ax", "grp"), "th", None), P(("ax", "grp"), "th", None))
    return jax.shard_map(shards, mesh=mesh, in_specs=in_specs, out_specs=out_specs, check_vma=False)
```

```python
import functools

import jax
import jax.numpy as jnp
import numpy as np
from jax import lax
from jax.experimental import pallas as pl
from jax.experimental.pallas import tpu as pltpu
from jax.sharding import PartitionSpec as P

MESH = pl.DeviceIdType.MESH
F32 = jnp.float32
BF16 = jnp.bfloat16

X = 512
THETA = 384
R = 128
RW = 64
XL = 16
TL = 24
NT = 16
NA = 32

ADVECT_X = 0.08
ADVECT_T = 0.08
ADVECT_R = 0.15
LATERAL_U = 0.03
LATERAL_T = 0.04
LATERAL_W = 0.1
COUPLE_T = 0.6
COUPLE_W = 0.8


def folded_tables(points):
    spacing = 2.0 * np.pi / points
    offset = np.arange(points)[:, None] - np.arange(points)[None, :]
    parity = 1.0 - 2.0 * (offset % 2)
    angle = np.where(offset != 0, offset * 0.5 * spacing, 1.0)
    first = np.where(offset != 0, 0.5 * spacing * parity / np.tan(angle), 0.0)
    second = np.where(
        offset != 0,
        -parity * spacing**2 / (2.0 * np.sin(angle) ** 2),
        -(np.pi**2 / 3.0 + spacing**2 / 6.0),
    )
    half = points // 2
    parts = []
    for sign in (1.0, -1.0):
        both = np.concatenate(
            [0.5 * (table[:half, :half] + sign * table[:half, half:]) for table in (first, second)], axis=0
        ).astype(np.float32)
        high = both.astype(BF16)
        low = (both - high.astype(np.float32)).astype(BF16)
        parts.append(np.stack([high, low]))
    return np.stack(parts)


def split(value):
    high = value.astype(BF16)
    low = (value - high.astype(F32)).astype(BF16)
    return high, low


def dot(a, b):
    return jnp.dot(a, b, preferred_element_type=F32)


def dot_t(a, b):
    return lax.dot_general(a, b, (((1,), (1,)), ((), ())), preferred_element_type=F32)


def apply_inverse(matrix, value):
    m_high, m_low = split(matrix)
    high, low = split(value)
    return dot_t(
        jnp.concatenate([high, low, high], axis=1), jnp.concatenate([m_high, m_high, m_low], axis=1)
    )


def apply_folded(table, rows, top, bottom):
    results = []
    for which, value in ((0, top + bottom), (1, top - bottom)):
        high, low = split(value)
        t_high = table[which, 0, rows, :]
        t_low = table[which, 1, rows, :]
        results.append(dot(t_high, high) + dot(t_high, low) + dot(t_low, high))
    return results[0] + results[1], results[0] - results[1]


def kernel(
    fields_h, wall_h, fm_h, inv_h, wm_h, winv_h, ttab_h, xtab_h,
    done, rest, wdone,
    F, W, fm, inv, wm, winv, ttab, xtab,
    fT, WP, wT,
    Qt, Qx, Wt, Wx,
    Rt, Rx, WRt, WRx, Wn,
    cih, axh, cwh, awh,
    base, wbase,
    ld,
    sT, rT, sX, rX, sWT, rWT, sWX, rWX,
    bsT, brT, bsX, brX, bsWT, brWT, bsWX, brWX,
):
    ax = lax.axis_index("ax")
    th = lax.axis_index("th")
    grp = lax.axis_index("grp")
    a = ax * 2 + grp
    y = lax.div(ax, 2)
    core = lax.rem(ax, 2)
    xh = lax.div(th, 8)
    z = lax.rem(th, 8)
    odd_y = lax.rem(y, 2)
    x_wall = jnp.logical_and(core == 0, grp == odd_y)
    x_fluid = jnp.logical_not(x_wall)
    my_theta = 3 * y + core * (1 + grp)
    t_wall = xh == lax.rem(z, 2)

    barrier = pltpu.get_barrier_semaphore()

    def greet_t(k, _):
        pl.semaphore_signal(barrier, inc=1, device_id=(ax, lax.rem(th + k, NT), grp), device_id_type=MESH)
        return 0

    def greet_a(k, _):
        peer = lax.rem(a + k, NA)
        pl.semaphore_signal(
            barrier, inc=1, device_id=(lax.div(peer, 2), th, lax.rem(peer, 2)), device_id_type=MESH
        )
        return 0

    lax.fori_loop(1, NT, greet_t, 0)
    lax.fori_loop(1, NA, greet_a, 0)

    sources = (fields_h, wall_h, fm_h, inv_h, wm_h, winv_h, ttab_h, xtab_h)
    targets = (F, W, fm, inv, wm, winv, ttab, xtab)
    loads = [pltpu.make_async_copy(src, dst, ld.at[i]) for i, (src, dst) in enumerate(zip(sources, targets))]
    for load in loads:
        load.start()
    load_f, load_w, *load_rest = loads
    load_f.wait()

    F2 = F.reshape(4 * XL * TL, R)

    def turn(t, _):
        for c in range(4):
            fT[c // 2, t, c % 2] = F2[pl.ds(c * XL * TL + t, XL, stride=TL), :]
        return 0

    lax.fori_loop(0, TL, turn, 0)
    load_w.wait()
    for p in range(8):
        WP[p] = jnp.concatenate([W[p], W[p + 8]], axis=1)
    WP2 = WP.reshape(8 * TL, R)
    for t in range(TL):
        wT[t] = WP2[pl.ds(t, 8, stride=TL), :]

    pl.semaphore_wait(barrier, NT - 1 + NA - 1)

    def offset(i):
        return 4 + lax.div(i + 1, 2) * (1 - 2 * lax.rem(i, 2))

    def send(remote, src, dst, s_sem, r_sem, device):
        @pl.when(remote)
        def _():
            pltpu.make_async_remote_copy(
                src_ref=src, dst_ref=dst, send_sem=s_sem, recv_sem=r_sem, device_id=device, device_id_type=MESH
            ).start()

        @pl.when(jnp.logical_not(remote))
        def _():
            pltpu.make_async_copy(src, dst, r_sem).start()

    def theta_peer(i, flip):
        return lax.rem(xh + flip, 2) * 8 + lax.rem(z + offset(i), 8)

    def send_chunk(ch):
        def step(i, _):
            for flip in (1, 0):
                t = theta_peer(i, flip)
                send(
                    t != th, F.at[pl.ds(2 * ch, 2), t], Qt.at[pl.ds(2 * ch, 2), pl.ds(TL * th, TL)],
                    sT.at[ch], rT.at[ch], (ax, t, grp),
                )
            yy = lax.rem(y + offset(i), 8)
            for k in range(3):
                theta = 3 * yy + k
                c_to = (k + 1) // 2
                g_to = k // 2 + (1 - c_to) * (1 - lax.rem(yy, 2))
                a_to = 4 * yy + 2 * c_to + g_to
                send(
                    a_to != a, fT.at[ch, theta], Qx.at[pl.ds(2 * ch, 2), pl.ds(XL * a, XL)],
                    sX.at[ch], rX.at[ch], (2 * yy + c_to, th, g_to),
                )
            return 0

        lax.fori_loop(0, 8, step, 0)

    def send_wall():
        def step(i, _):
            p = lax.rem(z + offset(i), 8)
            t = lax.rem(p, 2) * 8 + p
            send(t != th, WP.at[p], Wt.at[pl.ds(TL * th, TL)], sWT, rWT, (ax, t, grp))
            yy = lax.rem(y + offset(i), 8)
            a_to = 4 * yy + lax.rem(yy, 2)
            send(
                a_to != a, wT.at[pl.ds(3 * yy, 3)], Wx.at[:, pl.ds(8 * a, 8)],
                sWX, rWX, (2 * yy, th, lax.rem(yy, 2)),
            )
            return 0

        lax.fori_loop(0, 8, step, 0)

    send_chunk(0)
    send_wall()
    send_chunk(1)

    for load in load_rest:
        load.wait()
    lane = lax.broadcasted_iota(jnp.int32, (TL, R), 1)
    m = fm[...]
    row_r = -0.5 * ADVECT_R * m
    row_lift = COUPLE_T * m * m
    wm2 = jnp.concatenate([wm[...], wm[...]], axis=1)
    row_wlift = COUPLE_W * wm2 * wm2

    kk = lax.broadcasted_iota(jnp.int32, (R, R), 0)
    jj = lax.broadcasted_iota(jnp.int32, (R, R), 1)
    spread = 1.0 / m
    spread_t = jnp.broadcast_to(spread, (R, R)).T
    beyond = jnp.sum(jnp.where(kk >= jj, spread_t, 0.0), axis=0, keepdims=True)
    total = jnp.sum(spread_t, axis=0, keepdims=True)
    radius = 1.0 - 0.5 * (beyond - 0.5 * spread) / total
    row_t1 = -ADVECT_T / radius
    row_t2 = 1.0 / (radius * radius)
    wspread = 1.0 / wm2
    wspread_t = jnp.broadcast_to(wspread, (R, R)).T
    within = jnp.sum(jnp.where(kk <= lax.rem(jj, RW), wspread_t, 0.0), axis=0, keepdims=True)
    wtotal = jnp.sum(jnp.where(kk < RW, wspread_t, 0.0), axis=0, keepdims=True)
    wradius = 1.0 + 0.2 * (within - 0.5 * wspread) / wtotal
    row_w2 = LATERAL_W / (wradius * wradius)

    def prepare(p, _):
        pair = WP[p]
        for h in range(2):
            x = p + 8 * h
            u_r = F[2, x] * row_r
            ghost = pltpu.roll(pair, 127 - 64 * h, axis=1)
            for c in range(4):
                q = F[c, x]
                edge = ghost if c == 3 else 0.0
                upper = jnp.where(lane == R - 1, edge, pltpu.roll(q, R - 1, axis=1))
                lower = jnp.where(lane == 0, q, pltpu.roll(q, 1, axis=1))
                value = q + u_r * (upper - lower)
                if c == 3:
                    value = value + jnp.where(lane == R - 1, row_lift * ghost, 0.0)
                base[c, x] = value
        last_0 = pltpu.roll(F[3, p], 1, axis=1)
        last_1 = pltpu.roll(F[3, p + 8], 65, axis=1)
        wbase[p] = pair + jnp.where(
            lane == 0, row_wlift * last_0, jnp.where(lane == RW, row_wlift * last_1, 0.0)
        )
        return 0

    lax.fori_loop(0, 8, prepare, 0)

    def full(ref, sem):
        pltpu.make_async_copy(ref, ref, sem).wait()

    half_t = THETA // 2
    half_x = X // 2

    def lam(ch, cc):
        return jnp.where(ch == 1, LATERAL_T, LATERAL_U) if cc == 1 else LATERAL_U

    def theta_chunk(ch):
        both = pl.ds(2 * ch, 2)
        full(Qt.at[both], rT.at[ch])
        top = jnp.concatenate([Qt[2 * ch, :half_t], Qt[2 * ch + 1, :half_t]], axis=1)
        bottom = jnp.concatenate([Qt[2 * ch, half_t:], Qt[2 * ch + 1, half_t:]], axis=1)
        firsts = apply_folded(ttab, slice(0, half_t), top, bottom)
        seconds = apply_folded(ttab, slice(half_t, THETA), top, bottom)
        for h in range(2):
            rows = slice(h * half_t, (h + 1) * half_t)
            swirl = Qt[1, rows] * row_t1
            for cc in range(2):
                cols = slice(cc * R, (cc + 1) * R)
                Rt[2 * ch + cc, rows] = swirl * firsts[h][:, cols] + seconds[h][:, cols] * (row_t2 * lam(ch, cc))

        def step(i, _):
            for flip in (1, 0):
                t = theta_peer(i, flip)
                send(
                    t != th, Rt.at[both, pl.ds(TL * t, TL)], cih.at[both, th], bsT.at[ch], brT.at[ch], (ax, t, grp)
                )
            return 0

        lax.fori_loop(0, 8, step, 0)

    def axial_chunk(ch):
        both = pl.ds(2 * ch, 2)
        full(Qx.at[both], rX.at[ch])
        top = jnp.concatenate([Qx[2 * ch, :half_x], Qx[2 * ch + 1, :half_x]], axis=1)
        bottom = jnp.concatenate([Qx[2 * ch, half_x:], Qx[2 * ch + 1, half_x:]], axis=1)
        firsts = apply_folded(xtab, slice(0, half_x), top, bottom)
        seconds = apply_folded(xtab, slice(half_x, X), top, bottom)
        for h in range(2):
            rows = slice(h * half_x, (h + 1) * half_x)
            stream = Qx[0, rows] * (-ADVECT_X)
            for cc in range(2):
                cols = slice(cc * R, (cc + 1) * R)
                Rx[2 * ch + cc, rows] = stream * firsts[h][:, cols] + seconds[h][:, cols] * lam(ch, cc)

        def step(i, _):
            yy = lax.rem(y + offset(i), 8)
            for k in range(4):
                a_to = 4 * yy + k
                send(
                    a_to != a, Rx.at[both, pl.ds(XL * a_to, XL)], axh.at[ch, my_theta],
                    bsX.at[ch], brX.at[ch], (2 * yy + k // 2, th, k % 2),
                )
            return 0

        lax.fori_loop(0, 8, step, 0)

    def theta_wall():
        full(Wt, rWT)
        seconds = apply_folded(ttab, slice(half_t, THETA), Wt[:half_t], Wt[half_t:])
        for h in range(2):
            WRt[h * half_t:(h + 1) * half_t] = seconds[h] * row_w2

        def step(i, _):
            for flip in (1, 0):
                t = theta_peer(i, flip)
                send(t != th, WRt.at[pl.ds(TL * t, TL)], cwh.at[z], bsWT, brWT, (ax, t, grp))
            return 0

        lax.fori_loop(0, 8, step, 0)

    low8 = lax.broadcasted_iota(jnp.int32, (8, R), 1) < RW

    def axial_wall():
        full(Wx, rWX)

        def unpack(s, _):
            rows = pl.ds(pl.multiple_of(8 * s, 8), 8)
            w0, w1, w2 = Wx[0, rows], Wx[1, rows], Wx[2, rows]
            even = pl.ds(pl.multiple_of(16 * s, 8), 8)
            odd = pl.ds(pl.multiple_of(16 * s + 8, 8), 8)
            Wn[even, 0:R] = jnp.where(low8, w0, pltpu.roll(w1, RW, axis=1))
            Wn[odd, 0:R] = jnp.where(low8, pltpu.roll(w0, RW, axis=1), w1)
            Wn[even, R:2 * R] = w2
            Wn[odd, R:2 * R] = pltpu.roll(w2, RW, axis=1)
            return 0

        lax.fori_loop(0, NA, unpack, 0)
        seconds = apply_folded(xtab, slice(half_x, X), Wn[:half_x], Wn[half_x:])
        for h in range(2):
            Wn[h * half_x:(h + 1) * half_x] = seconds[h] * LATERAL_W

        def pack(s, _):
            rows = pl.ds(pl.multiple_of(8 * s, 8), 8)
            even = pl.ds(pl.multiple_of(16 * s, 8), 8)
            odd = pl.ds(pl.multiple_of(16 * s + 8, 8), 8)
            e01, o01 = Wn[even, 0:R], Wn[odd, 0:R]
            WRx[0, rows] = jnp.where(low8, e01, pltpu.roll(o01, RW, axis=1))
            WRx[1, rows] = jnp.where(low8, pltpu.roll(e01, RW, axis=1), o01)
            WRx[2, rows] = jnp.where(low8, Wn[even, R:2 * R], pltpu.roll(Wn[odd, R:2 * R], RW, axis=1))
            return 0

        lax.fori_loop(0, NA, pack, 0)

        def step(i, _):
            yy = lax.rem(y + offset(i), 8)
            for k in range(4):
                a_to = 4 * yy + k
                send(
                    a_to != a, WRx.at[:, pl.ds(8 * a_to, 8)], awh.at[pl.ds(3 * y, 3)],
                    bsWX, brWX, (2 * yy + k // 2, th, k % 2),
                )
            return 0

        lax.fori_loop(0, 8, step, 0)

    theta_chunk(0)
    pl.when(x_fluid)(lambda: axial_chunk(0))
    pl.when(x_wall)(axial_wall)
    pl.when(t_wall)(theta_wall)
    theta_chunk(1)
    pl.when(x_fluid)(lambda: axial_chunk(1))

    axh2 = axh.reshape(4 * XL * TL, R)

    def gather(ch, out):
        full(cih.at[pl.ds(2 * ch, 2)], brT.at[ch])
        full(axh.at[ch], brX.at[ch])

        def add(x, _):
            for cc in range(2):
                c = 2 * ch + cc
                axial = axh2[pl.ds(ch * 2 * XL * TL + cc * XL + x, TL, stride=2 * XL), :]
                out[cc, x] = base[c, x] + cih[c, x] + axial
            return 0

        lax.fori_loop(0, XL, add, 0)

    gather(0, done)
    for c in range(2):
        done[c] = apply_inverse(inv[0], done[c].reshape(XL * TL, R)).reshape(XL, TL, R)
    full(cwh, brWT)
    full(awh, brWX)
    awh2 = awh.reshape(8 * TL, R)

    def gather_wall(p, _):
        wbase[p] = wbase[p] + cwh[p] + awh2[pl.ds(p, TL, stride=8), :]
        return 0

    lax.fori_loop(0, 8, gather_wall, 0)
    value = wbase[...].reshape(8 * TL, R)
    nothing = jnp.zeros((RW, RW), F32)
    for h in range(2):
        pair = [winv[...], nothing] if h == 0 else [nothing, winv[...]]
        matrix = jnp.concatenate(pair, axis=1)
        wdone[8 * h:8 * h + 8] = apply_inverse(matrix, value).reshape(8, TL, RW)
    gather(1, rest)

    for ch in range(2):
        full(F.at[pl.ds(0, 2), pl.ds(0, NT - 1)], sT.at[ch])
        full(F.at[pl.ds(0, 2), pl.ds(0, NT - 1)], bsT.at[ch])

        @pl.when(x_fluid)
        def _():
            full(fT.at[ch, pl.ds(0, TL - 1)], sX.at[ch])
            full(Rx.at[pl.ds(0, 2), pl.ds(0, X - XL)], bsX.at[ch])

        @pl.when(x_wall)
        def _():
            full(fT.at[ch], sX.at[ch])

    @pl.when(t_wall)
    def _():
        full(WP.at[pl.ds(0, 7)], sWT)
        full(WRt.at[pl.ds(0, THETA - TL)], bsWT)

    @pl.when(jnp.logical_not(t_wall))
    def _():
        full(WP, sWT)

    @pl.when(x_wall)
    def _():
        full(wT.at[pl.ds(0, TL - 3)], sWX)
        full(WRx.at[:, pl.ds(0, 8 * (NA - 1))], bsWX)

    @pl.when(x_fluid)
    def _():
        full(wT, sWX)


def last_kernel(done, rest, wdone, inv, out_h, wout_h, buf, st):
    copies = [
        pltpu.make_async_copy(done, out_h.at[pl.ds(0, 2)], st.at[0]),
        pltpu.make_async_copy(wdone, wout_h, st.at[1]),
    ]
    for copy in copies:
        copy.start()
    for c in range(2):
        buf[c] = apply_inverse(inv[c], rest[c].reshape(XL * TL, R)).reshape(XL, TL, R)
        copy = pltpu.make_async_copy(buf.at[c], out_h.at[2 + c], st.at[2 + c])
        copy.start()
        copies.append(copy)
    for copy in copies:
        copy.wait()


def shards(fields, wall_temp, fluid_metric, fluid_radial_inverses, wall_metric, wall_inverse):
    vmem = pl.BlockSpec(memory_space=pltpu.VMEM)
    hbm = pl.BlockSpec(memory_space=pltpu.HBM)
    dma = pltpu.SemaphoreType.DMA
    ttab = jnp.asarray(folded_tables(THETA))
    xtab = jnp.asarray(folded_tables(X))

    def buf(*shape, dtype=F32):
        return pltpu.VMEM(shape, dtype)

    done, rest, wdone = pl.pallas_call(
        kernel,
        out_shape=(buf(2, XL, TL, R), buf(2, XL, TL, R), buf(XL, TL, RW)),
        in_specs=[hbm] * 8,
        out_specs=(vmem, vmem, vmem),
        scratch_shapes=[
            buf(4, XL, TL, R), buf(XL, TL, RW), buf(1, R), buf(2, R, R), buf(1, RW), buf(RW, RW),
            buf(*ttab.shape, dtype=BF16), buf(*xtab.shape, dtype=BF16),
            buf(2, TL, 2, XL, R), buf(8, TL, R), buf(TL, 8, R),
            buf(4, THETA, R), buf(4, X, R), buf(THETA, R), buf(3, X // 2, R),
            buf(4, THETA, R), buf(4, X, R), buf(THETA, R), buf(3, X // 2, R), buf(X, 2 * R),
            buf(4, XL, TL, R), buf(2, TL, 2, XL, R), buf(8, TL, R), buf(TL, 8, R),
            buf(4, XL, TL, R), buf(8, TL, R),
            dma((8,)),
            dma((2,)), dma((2,)), dma((2,)), dma((2,)), dma, dma, dma, dma,
            dma((2,)), dma((2,)), dma((2,)), dma((2,)), dma, dma, dma, dma,
        ],
        compiler_params=pltpu.CompilerParams(
            collective_id=0, has_side_effects=True, vmem_limit_bytes=40 * 2**20
        ),
    )(
        fields, wall_temp, fluid_metric.reshape(1, R), fluid_radial_inverses,
        wall_metric.reshape(1, RW), wall_inverse, ttab, xtab,
    )
    return pl.pallas_call(
        last_kernel,
        out_shape=(
            jax.ShapeDtypeStruct((4, XL, TL, R), F32),
            jax.ShapeDtypeStruct((XL, TL, RW), F32),
        ),
        in_specs=[vmem] * 4,
        out_specs=(hbm, hbm),
        scratch_shapes=[buf(2, XL, TL, R), dma((4,))],
        compiler_params=pltpu.CompilerParams(vmem_limit_bytes=16 * 2**20),
    )(done, rest, wdone, fluid_radial_inverses)


def solution(mesh):
    in_specs = (
        P(None, ("ax", "grp"), "th", None),
        P(("ax", "grp"), "th", None),
        P(),
        P(),
        P(),
        P(),
    )
    out_specs = (P(None, ("ax", "grp"), "th", None), P(("ax", "grp"), "th", None))
    return jax.shard_map(shards, mesh=mesh, in_specs=in_specs, out_specs=out_specs, check_vma=False)
```

```python
import functools

import jax
import jax.numpy as jnp
import numpy as np
from jax import lax
from jax.experimental import pallas as pl
from jax.experimental.pallas import tpu as pltpu
from jax.sharding import PartitionSpec as P

MESH = pl.DeviceIdType.MESH
F32 = jnp.float32
BF16 = jnp.bfloat16

X = 512
THETA = 384
R = 128
RW = 64
XL = 16
TL = 24
NT = 16
NA = 32

ADVECT_X = 0.08
ADVECT_T = 0.08
ADVECT_R = 0.15
LATERAL_U = 0.03
LATERAL_T = 0.04
LATERAL_W = 0.1
COUPLE_T = 0.6
COUPLE_W = 0.8


def folded_tables(points):
    spacing = 2.0 * np.pi / points
    offset = np.arange(points)[:, None] - np.arange(points)[None, :]
    parity = 1.0 - 2.0 * (offset % 2)
    angle = np.where(offset != 0, offset * 0.5 * spacing, 1.0)
    first = np.where(offset != 0, 0.5 * spacing * parity / np.tan(angle), 0.0)
    second = np.where(
        offset != 0,
        -parity * spacing**2 / (2.0 * np.sin(angle) ** 2),
        -(np.pi**2 / 3.0 + spacing**2 / 6.0),
    )
    half = points // 2
    parts = []
    for sign in (1.0, -1.0):
        both = np.concatenate(
            [0.5 * (table[:half, :half] + sign * table[:half, half:]) for table in (first, second)], axis=0
        ).astype(np.float32)
        high = both.astype(BF16)
        low = (both - high.astype(np.float32)).astype(BF16)
        parts.append(np.stack([high, low]))
    return np.stack(parts)


def split(value):
    high = value.astype(BF16)
    low = (value - high.astype(F32)).astype(BF16)
    return high, low


def dot(a, b):
    return jnp.dot(a, b, preferred_element_type=F32)


def dot_t(a, b):
    return lax.dot_general(a, b, (((1,), (1,)), ((), ())), preferred_element_type=F32)


def inverse_parts(matrix):
    high, low = split(matrix)
    return jnp.concatenate([high, high, low], axis=1)


def apply_inverse(parts, value):
    high, low = split(value)
    return dot_t(jnp.concatenate([high, low, high], axis=1), parts)


def apply_folded(table, rows, top, bottom):
    results = []
    for which, value in ((0, top + bottom), (1, top - bottom)):
        high, low = split(value)
        t_high = table[which, 0, rows, :]
        t_low = table[which, 1, rows, :]
        results.append(dot(t_high, high) + dot(t_high, low) + dot(t_low, high))
    return results[0] + results[1], results[0] - results[1]


def kernel(
    fields_h, wall_h, fm_h, inv_h, wm_h, winv_h, ttab_h, xtab_h,
    done, rest, wdone, parts,
    F, W, fm, inv, wm, winv, ttab, xtab,
    fT, WP, wT,
    Qt, Qx, Wt, Wx,
    Rt, Rx, WRt, WRx, Wn,
    cih, axh, cwh, awh,
    base, wbase,
    ld,
    sT, rT, sX, rX, sWT, rWT, sWX, rWX,
    bsT, brT, bsX, brX, bsWT, brWT, bsWX, brWX,
):
    ax = lax.axis_index("ax")
    th = lax.axis_index("th")
    grp = lax.axis_index("grp")
    a = ax * 2 + grp
    y = lax.div(ax, 2)
    core = lax.rem(ax, 2)
    xh = lax.div(th, 8)
    z = lax.rem(th, 8)
    odd_y = lax.rem(y, 2)
    x_wall = jnp.logical_and(core == 0, grp == odd_y)
    x_fluid = jnp.logical_not(x_wall)
    my_theta = 3 * y + core * (1 + grp)
    t_wall = xh == lax.rem(z, 2)

    barrier = pltpu.get_barrier_semaphore()

    def greet_t(k, _):
        pl.semaphore_signal(barrier, inc=1, device_id=(ax, lax.rem(th + k, NT), grp), device_id_type=MESH)
        return 0

    def greet_a(k, _):
        peer = lax.rem(a + k, NA)
        pl.semaphore_signal(
            barrier, inc=1, device_id=(lax.div(peer, 2), th, lax.rem(peer, 2)), device_id_type=MESH
        )
        return 0

    lax.fori_loop(1, NT, greet_t, 0)
    lax.fori_loop(1, NA, greet_a, 0)

    sources = (fields_h, wall_h, fm_h, inv_h, wm_h, winv_h, ttab_h, xtab_h)
    targets = (F, W, fm, inv, wm, winv, ttab, xtab)
    loads = [pltpu.make_async_copy(src, dst, ld.at[i]) for i, (src, dst) in enumerate(zip(sources, targets))]
    for load in loads:
        load.start()
    load_f, load_w, *load_rest = loads
    load_f.wait()

    F2 = F.reshape(4 * XL * TL, R)

    def turn(t, _):
        for c in range(4):
            fT[c // 2, t, c % 2] = F2[pl.ds(c * XL * TL + t, XL, stride=TL), :]
        return 0

    lax.fori_loop(0, TL, turn, 0)
    load_w.wait()
    for p in range(8):
        WP[p] = jnp.concatenate([W[p], W[p + 8]], axis=1)
    WP2 = WP.reshape(8 * TL, R)
    for t in range(TL):
        wT[t] = WP2[pl.ds(t, 8, stride=TL), :]

    pl.semaphore_wait(barrier, NT - 1 + NA - 1)

    def offset(i):
        return 4 + lax.div(i + 1, 2) * (1 - 2 * lax.rem(i, 2))

    def send(remote, src, dst, s_sem, r_sem, device):
        @pl.when(remote)
        def _():
            pltpu.make_async_remote_copy(
                src_ref=src, dst_ref=dst, send_sem=s_sem, recv_sem=r_sem, device_id=device, device_id_type=MESH
            ).start()

        @pl.when(jnp.logical_not(remote))
        def _():
            pltpu.make_async_copy(src, dst, r_sem).start()

    def theta_peer(i, flip):
        return lax.rem(xh + flip, 2) * 8 + lax.rem(z + offset(i), 8)

    def send_chunk(ch):
        def step(i, _):
            for flip in (1, 0):
                t = theta_peer(i, flip)
                send(
                    t != th, F.at[pl.ds(2 * ch, 2), t], Qt.at[pl.ds(2 * ch, 2), pl.ds(TL * th, TL)],
                    sT.at[ch], rT.at[ch], (ax, t, grp),
                )
            yy = lax.rem(y + offset(i), 8)
            for k in range(3):
                theta = 3 * yy + k
                c_to = (k + 1) // 2
                g_to = k // 2 + (1 - c_to) * (1 - lax.rem(yy, 2))
                a_to = 4 * yy + 2 * c_to + g_to
                send(
                    a_to != a, fT.at[ch, theta], Qx.at[pl.ds(2 * ch, 2), pl.ds(XL * a, XL)],
                    sX.at[ch], rX.at[ch], (2 * yy + c_to, th, g_to),
                )
            return 0

        lax.fori_loop(0, 8, step, 0)

    def send_wall():
        def step(i, _):
            p = lax.rem(z + offset(i), 8)
            t = lax.rem(p, 2) * 8 + p
            send(t != th, WP.at[p], Wt.at[pl.ds(TL * th, TL)], sWT, rWT, (ax, t, grp))
            yy = lax.rem(y + offset(i), 8)
            a_to = 4 * yy + lax.rem(yy, 2)
            send(
                a_to != a, wT.at[pl.ds(3 * yy, 3)], Wx.at[:, pl.ds(8 * a, 8)],
                sWX, rWX, (2 * yy, th, lax.rem(yy, 2)),
            )
            return 0

        lax.fori_loop(0, 8, step, 0)

    send_chunk(0)
    send_wall()
    send_chunk(1)

    for load in load_rest:
        load.wait()
    lane = lax.broadcasted_iota(jnp.int32, (TL, R), 1)
    m = fm[...]
    row_r = -0.5 * ADVECT_R * m
    row_lift = COUPLE_T * m * m
    wm2 = jnp.concatenate([wm[...], wm[...]], axis=1)
    row_wlift = COUPLE_W * wm2 * wm2

    kk = lax.broadcasted_iota(jnp.int32, (R, R), 0)
    jj = lax.broadcasted_iota(jnp.int32, (R, R), 1)
    spread = 1.0 / m
    spread_t = jnp.broadcast_to(spread, (R, R)).T
    beyond = jnp.sum(jnp.where(kk >= jj, spread_t, 0.0), axis=0, keepdims=True)
    total = jnp.sum(spread_t, axis=0, keepdims=True)
    radius = 1.0 - 0.5 * (beyond - 0.5 * spread) / total
    row_t1 = -ADVECT_T / radius
    row_t2 = 1.0 / (radius * radius)
    wspread = 1.0 / wm2
    wspread_t = jnp.broadcast_to(wspread, (R, R)).T
    within = jnp.sum(jnp.where(kk <= lax.rem(jj, RW), wspread_t, 0.0), axis=0, keepdims=True)
    wtotal = jnp.sum(jnp.where(kk < RW, wspread_t, 0.0), axis=0, keepdims=True)
    wradius = 1.0 + 0.2 * (within - 0.5 * wspread) / wtotal
    row_w2 = LATERAL_W / (wradius * wradius)

    def prepare(p, _):
        pair = WP[p]
        for h in range(2):
            x = p + 8 * h
            u_r = F[2, x] * row_r
            ghost = pltpu.roll(pair, 127 - 64 * h, axis=1)
            for c in range(4):
                q = F[c, x]
                edge = ghost if c == 3 else 0.0
                upper = jnp.where(lane == R - 1, edge, pltpu.roll(q, R - 1, axis=1))
                lower = jnp.where(lane == 0, q, pltpu.roll(q, 1, axis=1))
                value = q + u_r * (upper - lower)
                if c == 3:
                    value = value + jnp.where(lane == R - 1, row_lift * ghost, 0.0)
                base[c, x] = value
        last_0 = pltpu.roll(F[3, p], 1, axis=1)
        last_1 = pltpu.roll(F[3, p + 8], 65, axis=1)
        wbase[p] = pair + jnp.where(
            lane == 0, row_wlift * last_0, jnp.where(lane == RW, row_wlift * last_1, 0.0)
        )
        return 0

    lax.fori_loop(0, 8, prepare, 0)
    for i in range(2):
        parts[i] = inverse_parts(inv[i])

    def full(ref, sem):
        pltpu.make_async_copy(ref, ref, sem).wait()

    half_t = THETA // 2
    half_x = X // 2

    def lam(ch, cc):
        return jnp.where(ch == 1, LATERAL_T, LATERAL_U) if cc == 1 else LATERAL_U

    def theta_chunk(ch):
        both = pl.ds(2 * ch, 2)
        full(Qt.at[both], rT.at[ch])
        top = jnp.concatenate([Qt[2 * ch, :half_t], Qt[2 * ch + 1, :half_t]], axis=1)
        bottom = jnp.concatenate([Qt[2 * ch, half_t:], Qt[2 * ch + 1, half_t:]], axis=1)
        firsts = apply_folded(ttab, slice(0, half_t), top, bottom)
        seconds = apply_folded(ttab, slice(half_t, THETA), top, bottom)
        for h in range(2):
            rows = slice(h * half_t, (h + 1) * half_t)
            swirl = Qt[1, rows] * row_t1
            for cc in range(2):
                cols = slice(cc * R, (cc + 1) * R)
                Rt[2 * ch + cc, rows] = swirl * firsts[h][:, cols] + seconds[h][:, cols] * (row_t2 * lam(ch, cc))

        def step(i, _):
            for flip in (1, 0):
                t = theta_peer(i, flip)
                send(
                    t != th, Rt.at[both, pl.ds(TL * t, TL)], cih.at[both, th], bsT.at[ch], brT.at[ch], (ax, t, grp)
                )
            return 0

        lax.fori_loop(0, 8, step, 0)

    def axial_chunk(ch):
        both = pl.ds(2 * ch, 2)
        full(Qx.at[both], rX.at[ch])
        top = jnp.concatenate([Qx[2 * ch, :half_x], Qx[2 * ch + 1, :half_x]], axis=1)
        bottom = jnp.concatenate([Qx[2 * ch, half_x:], Qx[2 * ch + 1, half_x:]], axis=1)
        firsts = apply_folded(xtab, slice(0, half_x), top, bottom)
        seconds = apply_folded(xtab, slice(half_x, X), top, bottom)
        for h in range(2):
            rows = slice(h * half_x, (h + 1) * half_x)
            stream = Qx[0, rows] * (-ADVECT_X)
            for cc in range(2):
                cols = slice(cc * R, (cc + 1) * R)
                Rx[2 * ch + cc, rows] = stream * firsts[h][:, cols] + seconds[h][:, cols] * lam(ch, cc)

        def step(i, _):
            yy = lax.rem(y + offset(i), 8)
            for k in range(4):
                a_to = 4 * yy + k
                send(
                    a_to != a, Rx.at[both, pl.ds(XL * a_to, XL)], axh.at[ch, my_theta],
                    bsX.at[ch], brX.at[ch], (2 * yy + k // 2, th, k % 2),
                )
            return 0

        lax.fori_loop(0, 8, step, 0)

    def theta_wall():
        full(Wt, rWT)
        seconds = apply_folded(ttab, slice(half_t, THETA), Wt[:half_t], Wt[half_t:])
        for h in range(2):
            WRt[h * half_t:(h + 1) * half_t] = seconds[h] * row_w2

        def step(i, _):
            for flip in (1, 0):
                t = theta_peer(i, flip)
                send(t != th, WRt.at[pl.ds(TL * t, TL)], cwh.at[z], bsWT, brWT, (ax, t, grp))
            return 0

        lax.fori_loop(0, 8, step, 0)

    low8 = lax.broadcasted_iota(jnp.int32, (8, R), 1) < RW

    def axial_wall():
        full(Wx, rWX)

        def unpack(s, _):
            rows = pl.ds(pl.multiple_of(8 * s, 8), 8)
            w0, w1, w2 = Wx[0, rows], Wx[1, rows], Wx[2, rows]
            even = pl.ds(pl.multiple_of(16 * s, 8), 8)
            odd = pl.ds(pl.multiple_of(16 * s + 8, 8), 8)
            Wn[even, 0:R] = jnp.where(low8, w0, pltpu.roll(w1, RW, axis=1))
            Wn[odd, 0:R] = jnp.where(low8, pltpu.roll(w0, RW, axis=1), w1)
            Wn[even, R:2 * R] = w2
            Wn[odd, R:2 * R] = pltpu.roll(w2, RW, axis=1)
            return 0

        lax.fori_loop(0, NA, unpack, 0)
        seconds = apply_folded(xtab, slice(half_x, X), Wn[:half_x], Wn[half_x:])
        for h in range(2):
            Wn[h * half_x:(h + 1) * half_x] = seconds[h] * LATERAL_W

        def pack(s, _):
            rows = pl.ds(pl.multiple_of(8 * s, 8), 8)
            even = pl.ds(pl.multiple_of(16 * s, 8), 8)
            odd = pl.ds(pl.multiple_of(16 * s + 8, 8), 8)
            e01, o01 = Wn[even, 0:R], Wn[odd, 0:R]
            WRx[0, rows] = jnp.where(low8, e01, pltpu.roll(o01, RW, axis=1))
            WRx[1, rows] = jnp.where(low8, pltpu.roll(e01, RW, axis=1), o01)
            WRx[2, rows] = jnp.where(low8, Wn[even, R:2 * R], pltpu.roll(Wn[odd, R:2 * R], RW, axis=1))
            return 0

        lax.fori_loop(0, NA, pack, 0)

        def step(i, _):
            yy = lax.rem(y + offset(i), 8)
            for k in range(4):
                a_to = 4 * yy + k
                send(
                    a_to != a, WRx.at[:, pl.ds(8 * a_to, 8)], awh.at[pl.ds(3 * y, 3)],
                    bsWX, brWX, (2 * yy + k // 2, th, k % 2),
                )
            return 0

        lax.fori_loop(0, 8, step, 0)

    theta_chunk(0)
    pl.when(x_fluid)(lambda: axial_chunk(0))
    pl.when(x_wall)(axial_wall)
    pl.when(t_wall)(theta_wall)
    theta_chunk(1)
    pl.when(x_fluid)(lambda: axial_chunk(1))

    axh2 = axh.reshape(4 * XL * TL, R)

    def gather(ch, out):
        full(cih.at[pl.ds(2 * ch, 2)], brT.at[ch])
        full(axh.at[ch], brX.at[ch])

        def add(x, _):
            for cc in range(2):
                c = 2 * ch + cc
                axial = axh2[pl.ds(ch * 2 * XL * TL + cc * XL + x, TL, stride=2 * XL), :]
                out[cc, x] = base[c, x] + cih[c, x] + axial
            return 0

        lax.fori_loop(0, XL, add, 0)

    gather(0, done)
    for c in range(2):
        done[c] = apply_inverse(parts[0], done[c].reshape(XL * TL, R)).reshape(XL, TL, R)
    full(cwh, brWT)
    full(awh, brWX)
    awh2 = awh.reshape(8 * TL, R)

    def gather_wall(p, _):
        wbase[p] = wbase[p] + cwh[p] + awh2[pl.ds(p, TL, stride=8), :]
        return 0

    lax.fori_loop(0, 8, gather_wall, 0)
    value = wbase[...].reshape(8 * TL, R)
    nothing = jnp.zeros((RW, RW), F32)
    for h in range(2):
        pair = [winv[...], nothing] if h == 0 else [nothing, winv[...]]
        matrix = inverse_parts(jnp.concatenate(pair, axis=1))
        wdone[8 * h:8 * h + 8] = apply_inverse(matrix, value).reshape(8, TL, RW)
    gather(1, rest)

    for ch in range(2):
        full(F.at[pl.ds(0, 2), pl.ds(0, NT - 1)], sT.at[ch])
        full(F.at[pl.ds(0, 2), pl.ds(0, NT - 1)], bsT.at[ch])

        @pl.when(x_fluid)
        def _():
            full(fT.at[ch, pl.ds(0, TL - 1)], sX.at[ch])
            full(Rx.at[pl.ds(0, 2), pl.ds(0, X - XL)], bsX.at[ch])

        @pl.when(x_wall)
        def _():
            full(fT.at[ch], sX.at[ch])

    @pl.when(t_wall)
    def _():
        full(WP.at[pl.ds(0, 7)], sWT)
        full(WRt.at[pl.ds(0, THETA - TL)], bsWT)

    @pl.when(jnp.logical_not(t_wall))
    def _():
        full(WP, sWT)

    @pl.when(x_wall)
    def _():
        full(wT.at[pl.ds(0, TL - 3)], sWX)
        full(WRx.at[:, pl.ds(0, 8 * (NA - 1))], bsWX)

    @pl.when(x_fluid)
    def _():
        full(wT, sWX)


def last_kernel(done, rest, wdone, parts, out_h, wout_h, buf, st):
    copies = [
        pltpu.make_async_copy(done, out_h.at[pl.ds(0, 2)], st.at[0]),
        pltpu.make_async_copy(wdone, wout_h, st.at[1]),
    ]
    for copy in copies:
        copy.start()
    for c in range(2):
        buf[c] = apply_inverse(parts[c], rest[c].reshape(XL * TL, R)).reshape(XL, TL, R)
        copy = pltpu.make_async_copy(buf.at[c], out_h.at[2 + c], st.at[2 + c])
        copy.start()
        copies.append(copy)
    for copy in copies:
        copy.wait()


def shards(fields, wall_temp, fluid_metric, fluid_radial_inverses, wall_metric, wall_inverse):
    vmem = pl.BlockSpec(memory_space=pltpu.VMEM)
    hbm = pl.BlockSpec(memory_space=pltpu.HBM)
    dma = pltpu.SemaphoreType.DMA
    ttab = jnp.asarray(folded_tables(THETA))
    xtab = jnp.asarray(folded_tables(X))

    def buf(*shape, dtype=F32):
        return pltpu.VMEM(shape, dtype)

    done, rest, wdone, parts = pl.pallas_call(
        kernel,
        out_shape=(buf(2, XL, TL, R), buf(2, XL, TL, R), buf(XL, TL, RW), buf(2, R, 3 * R, dtype=BF16)),
        in_specs=[hbm] * 8,
        out_specs=(vmem,) * 4,
        scratch_shapes=[
            buf(4, XL, TL, R), buf(XL, TL, RW), buf(1, R), buf(2, R, R), buf(1, RW), buf(RW, RW),
            buf(*ttab.shape, dtype=BF16), buf(*xtab.shape, dtype=BF16),
            buf(2, TL, 2, XL, R), buf(8, TL, R), buf(TL, 8, R),
            buf(4, THETA, R), buf(4, X, R), buf(THETA, R), buf(3, X // 2, R),
            buf(4, THETA, R), buf(4, X, R), buf(THETA, R), buf(3, X // 2, R), buf(X, 2 * R),
            buf(4, XL, TL, R), buf(2, TL, 2, XL, R), buf(8, TL, R), buf(TL, 8, R),
            buf(4, XL, TL, R), buf(8, TL, R),
            dma((8,)),
            dma((2,)), dma((2,)), dma((2,)), dma((2,)), dma, dma, dma, dma,
            dma((2,)), dma((2,)), dma((2,)), dma((2,)), dma, dma, dma, dma,
        ],
        compiler_params=pltpu.CompilerParams(
            collective_id=0, has_side_effects=True, vmem_limit_bytes=64128 * 2**10
        ),
    )(
        fields, wall_temp, fluid_metric.reshape(1, R), fluid_radial_inverses,
        wall_metric.reshape(1, RW), wall_inverse, ttab, xtab,
    )
    return pl.pallas_call(
        last_kernel,
        out_shape=(
            jax.ShapeDtypeStruct((4, XL, TL, R), F32),
            jax.ShapeDtypeStruct((XL, TL, RW), F32),
        ),
        in_specs=[vmem] * 4,
        out_specs=(hbm, hbm),
        scratch_shapes=[buf(2, XL, TL, R), dma((4,))],
        compiler_params=pltpu.CompilerParams(vmem_limit_bytes=16 * 2**20),
    )(done, rest, wdone, parts)


def solution(mesh):
    in_specs = (
        P(None, ("ax", "grp"), "th", None),
        P(("ax", "grp"), "th", None),
        P(),
        P(),
        P(),
        P(),
    )
    out_specs = (P(None, ("ax", "grp"), "th", None), P(("ax", "grp"), "th", None))
    return jax.shard_map(shards, mesh=mesh, in_specs=in_specs, out_specs=out_specs, check_vma=False)
```

```python
import functools

import jax
import jax.numpy as jnp
import numpy as np
from jax import lax
from jax.experimental import pallas as pl
from jax.experimental.pallas import tpu as pltpu
from jax.sharding import PartitionSpec as P

MESH = pl.DeviceIdType.MESH
F32 = jnp.float32
BF16 = jnp.bfloat16

X = 512
THETA = 384
R = 128
RW = 64
XL = 16
TL = 24
NT = 16
NA = 32

ADVECT_X = 0.08
ADVECT_T = 0.08
ADVECT_R = 0.15
LATERAL_U = 0.03
LATERAL_T = 0.04
LATERAL_W = 0.1
COUPLE_T = 0.6
COUPLE_W = 0.8


def folded_tables(points):
    spacing = 2.0 * np.pi / points
    offset = np.arange(points)[:, None] - np.arange(points)[None, :]
    parity = 1.0 - 2.0 * (offset % 2)
    angle = np.where(offset != 0, offset * 0.5 * spacing, 1.0)
    first = np.where(offset != 0, 0.5 * spacing * parity / np.tan(angle), 0.0)
    second = np.where(
        offset != 0,
        -parity * spacing**2 / (2.0 * np.sin(angle) ** 2),
        -(np.pi**2 / 3.0 + spacing**2 / 6.0),
    )
    half = points // 2
    parts = []
    for sign in (1.0, -1.0):
        both = np.concatenate(
            [0.5 * (table[:half, :half] + sign * table[:half, half:]) for table in (first, second)], axis=0
        ).astype(np.float32)
        high = both.astype(BF16)
        low = (both - high.astype(np.float32)).astype(BF16)
        parts.append(np.stack([high, low]))
    return np.stack(parts)


def split(value):
    high = value.astype(BF16)
    low = (value - high.astype(F32)).astype(BF16)
    return high, low


def dot(a, b):
    return jnp.dot(a, b, preferred_element_type=F32)


def dot_t(a, b):
    return lax.dot_general(a, b, (((1,), (1,)), ((), ())), preferred_element_type=F32)


def inverse_parts(matrix):
    high, low = split(matrix)
    return jnp.concatenate([high, high, low], axis=1)


def apply_inverse(parts, value):
    high, low = split(value)
    return dot_t(jnp.concatenate([high, low, high], axis=1), parts)


def apply_folded(table, rows, top, bottom):
    results = []
    for which, value in ((0, top + bottom), (1, top - bottom)):
        high, low = split(value)
        t_high = table[which, 0, rows, :]
        t_low = table[which, 1, rows, :]
        results.append(dot(t_high, high) + dot(t_high, low) + dot(t_low, high))
    return results[0] + results[1], results[0] - results[1]


def kernel(
    fields_h, wall_h, fm_h, inv_h, wm_h, winv_h, ttab_h, xtab_h,
    done, rest, wdone, parts,
    F, W, fm, inv, wm, winv, ttab, xtab,
    fT, WP, wT,
    Qt, Qx, Wt, Wx,
    Rt, Rx, WRt, WRx, Wn,
    cih, axh, cwh, awh,
    base, wbase,
    ld,
    sT, rT, sX, rX, sWT, rWT, sWX, rWX,
    bsT, brT, bsX, brX, bsWT, brWT, bsWX, brWX,
):
    ax = lax.axis_index("ax")
    th = lax.axis_index("th")
    grp = lax.axis_index("grp")
    a = ax * 2 + grp
    y = lax.div(ax, 2)
    core = lax.rem(ax, 2)
    xh = lax.div(th, 8)
    z = lax.rem(th, 8)
    x_whole = core == 0
    x_half = core == 1
    my_theta = 3 * y + 2 * grp
    t_wall = xh == lax.rem(z, 2)

    barrier = pltpu.get_barrier_semaphore()

    for far in (4, 3, 5, 2, 6, 1, 7, 0):
        for flip in (1, 0):
            if far or flip:
                peer = lax.rem(xh + flip, 2) * 8 + lax.rem(z + far, 8)
                pl.semaphore_signal(barrier, inc=1, device_id=(ax, peer, grp), device_id_type=MESH)
        for flip in range(4):
            if far or flip:
                peer = (2 * lax.rem(y + far, 8) + lax.rem(core + flip // 2, 2), th, lax.rem(grp + flip, 2))
                pl.semaphore_signal(barrier, inc=1, device_id=peer, device_id_type=MESH)

    sources = (fields_h, wall_h, fm_h, inv_h, wm_h, winv_h, ttab_h, xtab_h)
    targets = (F, W, fm, inv, wm, winv, ttab, xtab)
    loads = [pltpu.make_async_copy(src, dst, ld.at[i]) for i, (src, dst) in enumerate(zip(sources, targets))]
    for load in loads:
        load.start()
    load_f, load_w, *load_rest = loads
    load_f.wait()

    F2 = F.reshape(4 * XL * TL, R)

    def turn(t, _):
        for c in range(4):
            fT[c // 2, 2 * t + c % 2] = F2[pl.ds(c * XL * TL + t, XL, stride=TL), :]
        return 0

    lax.fori_loop(0, TL, turn, 0)
    low = lax.broadcasted_iota(jnp.int32, (XL, R), 1) < RW

    def swap_halves(ref, ch, yy):
        at = 6 * yy + 2
        one, two = ref[ch, at], ref[ch, at + 1]
        ref[ch, at] = jnp.where(low, one, pltpu.roll(two, RW, axis=1))
        ref[ch, at + 1] = jnp.where(low, pltpu.roll(one, RW, axis=1), two)

    def swap_all(ref, ch):
        def step(yy, _):
            swap_halves(ref, ch, yy)
            return 0

        lax.fori_loop(0, 8, step, 0)

    swap_all(fT, 0)
    swap_all(fT, 1)
    load_w.wait()
    for p in range(8):
        WP[p] = jnp.concatenate([W[p], W[p + 8]], axis=1)
    WP2 = WP.reshape(8 * TL, R)
    for t in range(TL):
        wT[t] = WP2[pl.ds(t, 8, stride=TL), :]

    pl.semaphore_wait(barrier, NT - 1 + NA - 1)

    def offset(i):
        return 4 + lax.div(i + 1, 2) * (1 - 2 * lax.rem(i, 2))

    def send(remote, src, dst, s_sem, r_sem, device):
        @pl.when(remote)
        def _():
            pltpu.make_async_remote_copy(
                src_ref=src, dst_ref=dst, send_sem=s_sem, recv_sem=r_sem, device_id=device, device_id_type=MESH
            ).start()

        @pl.when(jnp.logical_not(remote))
        def _():
            pltpu.make_async_copy(src, dst, r_sem).start()

    def theta_peer(i, flip):
        return lax.rem(xh + flip, 2) * 8 + lax.rem(z + offset(i), 8)

    def send_chunk(ch):
        def step(i, _):
            for flip in (1, 0):
                t = theta_peer(i, flip)
                send(
                    t != th, F.at[pl.ds(2 * ch, 2), t], Qt.at[pl.ds(2 * ch, 2), pl.ds(TL * th, TL)],
                    sT.at[ch], rT.at[ch], (ax, t, grp),
                )
            yy = lax.rem(y + offset(i), 8)
            for g_to in range(2):
                a_to = 4 * yy + g_to
                send(
                    a_to != a, fT.at[ch, pl.ds(6 * yy + 4 * g_to, 2)], Qx.at[pl.ds(2 * ch, 2), pl.ds(XL * a, XL)],
                    sX.at[ch], rX.at[ch], (2 * yy, th, g_to),
                )
                send(
                    a_to + 2 != a, fT.at[ch, 6 * yy + 2 + g_to], Qx.at[ch, pl.ds(XL * a, XL)],
                    sX.at[ch], rX.at[ch], (2 * yy + 1, th, g_to),
                )
            return 0

        lax.fori_loop(0, 8, step, 0)

    def send_wall():
        def step(i, _):
            p = lax.rem(z + offset(i), 8)
            t = lax.rem(p, 2) * 8 + p
            send(t != th, WP.at[p], Wt.at[pl.ds(TL * th, TL)], sWT, rWT, (ax, t, grp))
            yy = lax.rem(y + offset(i), 8)
            for g_to in range(2):
                slots = pl.ds(0, 2 - g_to)
                send(
                    4 * yy + 2 + g_to != a, wT.at[pl.ds(3 * yy + 2 * g_to, 2 - g_to)], Wx.at[slots, pl.ds(8 * a, 8)],
                    sWX, rWX, (2 * yy + 1, th, g_to),
                )
            return 0

        lax.fori_loop(0, 8, step, 0)

    send_chunk(0)
    send_wall()
    send_chunk(1)

    for load in load_rest:
        load.wait()
    lane = lax.broadcasted_iota(jnp.int32, (TL, R), 1)
    m = fm[...]
    row_r = -0.5 * ADVECT_R * m
    row_lift = COUPLE_T * m * m
    wm2 = jnp.concatenate([wm[...], wm[...]], axis=1)
    row_wlift = COUPLE_W * wm2 * wm2

    kk = lax.broadcasted_iota(jnp.int32, (R, R), 0)
    jj = lax.broadcasted_iota(jnp.int32, (R, R), 1)
    spread = 1.0 / m
    spread_t = jnp.broadcast_to(spread, (R, R)).T
    beyond = jnp.sum(jnp.where(kk >= jj, spread_t, 0.0), axis=0, keepdims=True)
    total = jnp.sum(spread_t, axis=0, keepdims=True)
    radius = 1.0 - 0.5 * (beyond - 0.5 * spread) / total
    row_t1 = -ADVECT_T / radius
    row_t2 = 1.0 / (radius * radius)
    wspread = 1.0 / wm2
    wspread_t = jnp.broadcast_to(wspread, (R, R)).T
    within = jnp.sum(jnp.where(kk <= lax.rem(jj, RW), wspread_t, 0.0), axis=0, keepdims=True)
    wtotal = jnp.sum(jnp.where(kk < RW, wspread_t, 0.0), axis=0, keepdims=True)
    wradius = 1.0 + 0.2 * (within - 0.5 * wspread) / wtotal
    row_w2 = LATERAL_W / (wradius * wradius)

    def prepare(p, _):
        pair = WP[p]
        for h in range(2):
            x = p + 8 * h
            u_r = F[2, x] * row_r
            ghost = pltpu.roll(pair, 127 - 64 * h, axis=1)
            for c in range(4):
                q = F[c, x]
                edge = ghost if c == 3 else 0.0
                upper = jnp.where(lane == R - 1, edge, pltpu.roll(q, R - 1, axis=1))
                lower = jnp.where(lane == 0, q, pltpu.roll(q, 1, axis=1))
                value = q + u_r * (upper - lower)
                if c == 3:
                    value = value + jnp.where(lane == R - 1, row_lift * ghost, 0.0)
                base[c, x] = value
        last_0 = pltpu.roll(F[3, p], 1, axis=1)
        last_1 = pltpu.roll(F[3, p + 8], 65, axis=1)
        wbase[p] = pair + jnp.where(
            lane == 0, row_wlift * last_0, jnp.where(lane == RW, row_wlift * last_1, 0.0)
        )
        return 0

    lax.fori_loop(0, 8, prepare, 0)
    for i in range(2):
        parts[i] = inverse_parts(inv[i])

    def full(ref, sem):
        pltpu.make_async_copy(ref, ref, sem).wait()

    half_t = THETA // 2
    half_x = X // 2

    def lam(ch, cc):
        return jnp.where(ch == 1, LATERAL_T, LATERAL_U) if cc == 1 else LATERAL_U

    def theta_chunk(ch):
        both = pl.ds(2 * ch, 2)
        full(Qt.at[both], rT.at[ch])
        top = jnp.concatenate([Qt[2 * ch, :half_t], Qt[2 * ch + 1, :half_t]], axis=1)
        bottom = jnp.concatenate([Qt[2 * ch, half_t:], Qt[2 * ch + 1, half_t:]], axis=1)
        firsts = apply_folded(ttab, slice(0, half_t), top, bottom)
        seconds = apply_folded(ttab, slice(half_t, THETA), top, bottom)
        for h in range(2):
            rows = slice(h * half_t, (h + 1) * half_t)
            swirl = Qt[1, rows] * row_t1
            for cc in range(2):
                cols = slice(cc * R, (cc + 1) * R)
                Rt[2 * ch + cc, rows] = swirl * firsts[h][:, cols] + seconds[h][:, cols] * (row_t2 * lam(ch, cc))

        def step(i, _):
            for flip in (1, 0):
                t = theta_peer(i, flip)
                send(
                    t != th, Rt.at[both, pl.ds(TL * t, TL)], cih.at[both, th], bsT.at[ch], brT.at[ch], (ax, t, grp)
                )
            return 0

        lax.fori_loop(0, 8, step, 0)

    def axial_chunk(ch):
        both = pl.ds(2 * ch, 2)
        full(Qx.at[both], rX.at[ch])
        top = jnp.concatenate([Qx[2 * ch, :half_x], Qx[2 * ch + 1, :half_x]], axis=1)
        bottom = jnp.concatenate([Qx[2 * ch, half_x:], Qx[2 * ch + 1, half_x:]], axis=1)
        firsts = apply_folded(xtab, slice(0, half_x), top, bottom)
        seconds = apply_folded(xtab, slice(half_x, X), top, bottom)
        for h in range(2):
            rows = slice(h * half_x, (h + 1) * half_x)
            stream = Qx[0, rows] * (-ADVECT_X)
            for cc in range(2):
                cols = slice(cc * R, (cc + 1) * R)
                Rx[2 * ch + cc, rows] = stream * firsts[h][:, cols] + seconds[h][:, cols] * lam(ch, cc)

        def step(i, _):
            yy = lax.rem(y + offset(i), 8)
            for k in range(4):
                a_to = 4 * yy + k
                send(
                    a_to != a, Rx.at[both, pl.ds(XL * a_to, XL)], axh.at[ch, pl.ds(2 * my_theta, 2)],
                    bsX.at[ch], brX.at[ch], (2 * yy + k // 2, th, k % 2),
                )
            return 0

        lax.fori_loop(0, 8, step, 0)

    lam_halves = jnp.where(lane[:1] < RW, LATERAL_U, LATERAL_T)

    def axial_half(ch):
        full(Qx.at[ch], rX.at[ch])
        firsts = apply_folded(xtab, slice(0, half_x), Qx[ch, :half_x], Qx[ch, half_x:])
        seconds = apply_folded(xtab, slice(half_x, X), Qx[ch, :half_x], Qx[ch, half_x:])
        lam_row = jnp.where(ch == 1, lam_halves, LATERAL_U)
        low_x = lax.broadcasted_iota(jnp.int32, (half_x, R), 1) < RW
        for h in range(2):
            rows = slice(h * half_x, (h + 1) * half_x)
            stream = Qx[0, rows] * (-ADVECT_X)
            stream = jnp.where(low_x, stream, pltpu.roll(stream, RW, axis=1))
            Rx[ch, rows] = stream * firsts[h] + seconds[h] * lam_row

        def step(i, _):
            yy = lax.rem(y + offset(i), 8)
            for k in range(4):
                a_to = 4 * yy + k
                send(
                    a_to != a, Rx.at[ch, pl.ds(XL * a_to, XL)], axh.at[ch, 6 * y + 2 + grp],
                    bsX.at[ch], brX.at[ch], (2 * yy + k // 2, th, k % 2),
                )
            return 0

        lax.fori_loop(0, 8, step, 0)

    def theta_wall():
        full(Wt, rWT)
        seconds = apply_folded(ttab, slice(half_t, THETA), Wt[:half_t], Wt[half_t:])
        for h in range(2):
            WRt[h * half_t:(h + 1) * half_t] = seconds[h] * row_w2

        def step(i, _):
            for flip in (1, 0):
                t = theta_peer(i, flip)
                send(t != th, WRt.at[pl.ds(TL * t, TL)], cwh.at[z], bsWT, brWT, (ax, t, grp))
            return 0

        lax.fori_loop(0, 8, step, 0)

    low8 = lax.broadcasted_iota(jnp.int32, (8, R), 1) < RW

    def axial_wall(g):
        slots = pl.ds(0, 2 - g)
        full(Wx.at[slots], rWX)

        def unpack(s, _):
            rows = pl.ds(pl.multiple_of(8 * s, 8), 8)
            even = pl.ds(pl.multiple_of(16 * s, 8), 8)
            odd = pl.ds(pl.multiple_of(16 * s + 8, 8), 8)
            w0 = Wx[0, rows]
            w1 = Wx[1 - g, rows]
            Wn[even] = jnp.where(low8, w0, pltpu.roll(w1, RW, axis=1))
            Wn[odd] = jnp.where(low8, pltpu.roll(w0, RW, axis=1), w1)
            return 0

        lax.fori_loop(0, NA, unpack, 0)
        seconds = apply_folded(xtab, slice(half_x, X), Wn[:half_x], Wn[half_x:])
        for h in range(2):
            Wn[h * half_x:(h + 1) * half_x] = seconds[h] * LATERAL_W

        def pack(s, _):
            rows = pl.ds(pl.multiple_of(8 * s, 8), 8)
            even = Wn[pl.ds(pl.multiple_of(16 * s, 8), 8)]
            odd = Wn[pl.ds(pl.multiple_of(16 * s + 8, 8), 8)]
            WRx[0, rows] = jnp.where(low8, even, pltpu.roll(odd, RW, axis=1))
            if g == 0:
                WRx[1, rows] = jnp.where(low8, pltpu.roll(even, RW, axis=1), odd)
            return 0

        lax.fori_loop(0, NA, pack, 0)

        def step(i, _):
            yy = lax.rem(y + offset(i), 8)
            for k in range(4):
                a_to = 4 * yy + k
                send(
                    a_to != a, WRx.at[slots, pl.ds(8 * a_to, 8)], awh.at[pl.ds(3 * y + 2 * g, 2 - g)],
                    bsWX, brWX, (2 * yy + k // 2, th, k % 2),
                )
            return 0

        lax.fori_loop(0, 8, step, 0)

    theta_chunk(0)
    pl.when(x_whole)(lambda: axial_chunk(0))
    pl.when(x_half)(lambda: axial_half(0))
    pl.when(jnp.logical_and(x_half, grp == 0))(lambda: axial_wall(0))
    pl.when(jnp.logical_and(x_half, grp == 1))(lambda: axial_wall(1))
    pl.when(t_wall)(theta_wall)
    theta_chunk(1)
    pl.when(x_whole)(lambda: axial_chunk(1))
    pl.when(x_half)(lambda: axial_half(1))

    axh2 = axh.reshape(4 * XL * TL, R)

    def gather(ch, out):
        full(cih.at[pl.ds(2 * ch, 2)], brT.at[ch])
        full(axh.at[ch], brX.at[ch])
        swap_all(axh, ch)

        def add(x, _):
            for cc in range(2):
                c = 2 * ch + cc
                axial = axh2[pl.ds(ch * 2 * XL * TL + cc * XL + x, TL, stride=2 * XL), :]
                out[cc, x] = base[c, x] + cih[c, x] + axial
            return 0

        lax.fori_loop(0, XL, add, 0)

    gather(0, done)
    for c in range(2):
        done[c] = apply_inverse(parts[0], done[c].reshape(XL * TL, R)).reshape(XL, TL, R)
    full(cwh, brWT)
    full(awh, brWX)
    awh2 = awh.reshape(8 * TL, R)

    def gather_wall(p, _):
        wbase[p] = wbase[p] + cwh[p] + awh2[pl.ds(p, TL, stride=8), :]
        return 0

    lax.fori_loop(0, 8, gather_wall, 0)
    value = wbase[...].reshape(8 * TL, R)
    nothing = jnp.zeros((RW, RW), F32)
    for h in range(2):
        pair = [winv[...], nothing] if h == 0 else [nothing, winv[...]]
        matrix = inverse_parts(jnp.concatenate(pair, axis=1))
        wdone[8 * h:8 * h + 8] = apply_inverse(matrix, value).reshape(8, TL, RW)
    gather(1, rest)

    for ch in range(2):
        full(F.at[pl.ds(0, 2), pl.ds(0, NT - 1)], sT.at[ch])
        full(F.at[pl.ds(0, 2), pl.ds(0, NT - 1)], bsT.at[ch])

        @pl.when(x_whole)
        def _():
            full(fT.at[ch, pl.ds(0, 2 * TL - 2)], sX.at[ch])
            full(Rx.at[pl.ds(0, 2), pl.ds(0, X - XL)], bsX.at[ch])

        @pl.when(x_half)
        def _():
            full(fT.at[ch, pl.ds(0, 2 * TL - 1)], sX.at[ch])
            full(Rx.at[0, pl.ds(0, X - XL)], bsX.at[ch])

    @pl.when(t_wall)
    def _():
        full(WP.at[pl.ds(0, 7)], sWT)
        full(WRt.at[pl.ds(0, THETA - TL)], bsWT)

    @pl.when(jnp.logical_not(t_wall))
    def _():
        full(WP, sWT)

    @pl.when(x_whole)
    def _():
        full(wT, sWX)

    for g in range(2):
        @pl.when(jnp.logical_and(x_half, grp == g))
        def _():
            full(wT.at[pl.ds(0, TL - 2 + g)], sWX)
            full(WRx.at[pl.ds(0, 2 - g), pl.ds(0, 8 * (NA - 1))], bsWX)


def last_kernel(done, rest, wdone, parts, out_h, wout_h, buf, st):
    copies = [
        pltpu.make_async_copy(done, out_h.at[pl.ds(0, 2)], st.at[0]),
        pltpu.make_async_copy(wdone, wout_h, st.at[1]),
    ]
    for copy in copies:
        copy.start()
    for c in range(2):
        buf[c] = apply_inverse(parts[c], rest[c].reshape(XL * TL, R)).reshape(XL, TL, R)
        copy = pltpu.make_async_copy(buf.at[c], out_h.at[2 + c], st.at[2 + c])
        copy.start()
        copies.append(copy)
    for copy in copies:
        copy.wait()


def shards(fields, wall_temp, fluid_metric, fluid_radial_inverses, wall_metric, wall_inverse):
    vmem = pl.BlockSpec(memory_space=pltpu.VMEM)
    hbm = pl.BlockSpec(memory_space=pltpu.HBM)
    dma = pltpu.SemaphoreType.DMA
    ttab = jnp.asarray(folded_tables(THETA))
    xtab = jnp.asarray(folded_tables(X))

    def buf(*shape, dtype=F32):
        return pltpu.VMEM(shape, dtype)

    done, rest, wdone, parts = pl.pallas_call(
        kernel,
        out_shape=(buf(2, XL, TL, R), buf(2, XL, TL, R), buf(XL, TL, RW), buf(2, R, 3 * R, dtype=BF16)),
        in_specs=[hbm] * 8,
        out_specs=(vmem,) * 4,
        scratch_shapes=[
            buf(4, XL, TL, R), buf(XL, TL, RW), buf(1, R), buf(2, R, R), buf(1, RW), buf(RW, RW),
            buf(*ttab.shape, dtype=BF16), buf(*xtab.shape, dtype=BF16),
            buf(2, 2 * TL, XL, R), buf(8, TL, R), buf(TL, 8, R),
            buf(4, THETA, R), buf(4, X, R), buf(THETA, R), buf(2, X // 2, R),
            buf(4, THETA, R), buf(4, X, R), buf(THETA, R), buf(2, X // 2, R), buf(X, R),
            buf(4, XL, TL, R), buf(2, 2 * TL, XL, R), buf(8, TL, R), buf(TL, 8, R),
            buf(4, XL, TL, R), buf(8, TL, R),
            dma((8,)),
            dma((2,)), dma((2,)), dma((2,)), dma((2,)), dma, dma, dma, dma,
            dma((2,)), dma((2,)), dma((2,)), dma((2,)), dma, dma, dma, dma,
        ],
        compiler_params=pltpu.CompilerParams(
            collective_id=0, has_side_effects=True, vmem_limit_bytes=64128 * 2**10
        ),
    )(
        fields, wall_temp, fluid_metric.reshape(1, R), fluid_radial_inverses,
        wall_metric.reshape(1, RW), wall_inverse, ttab, xtab,
    )
    return pl.pallas_call(
        last_kernel,
        out_shape=(
            jax.ShapeDtypeStruct((4, XL, TL, R), F32),
            jax.ShapeDtypeStruct((XL, TL, RW), F32),
        ),
        in_specs=[vmem] * 4,
        out_specs=(hbm, hbm),
        scratch_shapes=[buf(2, XL, TL, R), dma((4,))],
        compiler_params=pltpu.CompilerParams(vmem_limit_bytes=16 * 2**20),
    )(done, rest, wdone, parts)


def solution(mesh):
    in_specs = (
        P(None, ("ax", "grp"), "th", None),
        P(("ax", "grp"), "th", None),
        P(),
        P(),
        P(),
        P(),
    )
    out_specs = (P(None, ("ax", "grp"), "th", None), P(("ax", "grp"), "th", None))
    return jax.shard_map(shards, mesh=mesh, in_specs=in_specs, out_specs=out_specs, check_vma=False)
```

```python
import functools

import jax
import jax.numpy as jnp
import numpy as np
from jax import lax
from jax.experimental import pallas as pl
from jax.experimental.pallas import tpu as pltpu
from jax.sharding import PartitionSpec as P

MESH = pl.DeviceIdType.MESH
F32 = jnp.float32
BF16 = jnp.bfloat16

X = 512
THETA = 384
R = 128
RW = 64
XL = 16
TL = 24
NT = 16
NA = 32

ADVECT_X = 0.08
ADVECT_T = 0.08
ADVECT_R = 0.15
LATERAL_U = 0.03
LATERAL_T = 0.04
LATERAL_W = 0.1
COUPLE_T = 0.6
COUPLE_W = 0.8


def folded_tables(points):
    spacing = 2.0 * np.pi / points
    offset = np.arange(points)[:, None] - np.arange(points)[None, :]
    parity = 1.0 - 2.0 * (offset % 2)
    angle = np.where(offset != 0, offset * 0.5 * spacing, 1.0)
    first = np.where(offset != 0, 0.5 * spacing * parity / np.tan(angle), 0.0)
    second = np.where(
        offset != 0,
        -parity * spacing**2 / (2.0 * np.sin(angle) ** 2),
        -(np.pi**2 / 3.0 + spacing**2 / 6.0),
    )
    half = points // 2
    parts = []
    for sign in (1.0, -1.0):
        both = np.concatenate(
            [0.5 * (table[:half, :half] + sign * table[:half, half:]) for table in (first, second)], axis=0
        ).astype(np.float32)
        high = both.astype(BF16)
        low = (both - high.astype(np.float32)).astype(BF16)
        parts.append(np.stack([high, low]))
    return np.stack(parts)


def split(value):
    high = value.astype(BF16)
    low = (value - high.astype(F32)).astype(BF16)
    return high, low


def dot(a, b):
    return jnp.dot(a, b, preferred_element_type=F32)


def dot_t(a, b):
    return lax.dot_general(a, b, (((1,), (1,)), ((), ())), preferred_element_type=F32)


def inverse_parts(matrix):
    high, low = split(matrix)
    return jnp.concatenate([high, high, low], axis=1)


def apply_inverse(parts, value):
    high, low = split(value)
    return dot_t(jnp.concatenate([high, low, high], axis=1), parts)


def apply_folded(table, rows, top, bottom):
    results = []
    for which, value in ((0, top + bottom), (1, top - bottom)):
        high, low = split(value)
        t_high = table[which, 0, rows, :]
        t_low = table[which, 1, rows, :]
        results.append(dot(t_high, high) + dot(t_high, low) + dot(t_low, high))
    return results[0] + results[1], results[0] - results[1]


def kernel(
    fields_h, wall_h, fm_h, inv_h, wm_h, winv_h, ttab_h, xtab_h,
    done, rest, wdone, parts,
    F, W, fm, inv, wm, winv, ttab, xtab,
    fT, WP, wT,
    Qt, Qx, Wt, Wx,
    Rt, Rx, WRt, WRx, Wn,
    cih, axh, cwh, awh,
    base, wbase,
    ld,
    sT, rT, sX, rX, sWT, rWT, sWX, rWX,
    bsT, brT, bsX, brX, bsWT, brWT, bsWX, brWX,
):
    ax = lax.axis_index("ax")
    th = lax.axis_index("th")
    grp = lax.axis_index("grp")
    a = ax * 2 + grp
    y = lax.div(ax, 2)
    core = lax.rem(ax, 2)
    xh = lax.div(th, 8)
    z = lax.rem(th, 8)
    x_whole = core == 0
    x_half = core == 1
    my_theta = 3 * y + 2 * grp
    t_wall = xh == lax.rem(z, 2)

    barrier = pltpu.get_barrier_semaphore()

    for far in (4, 3, 5, 2, 6, 1, 7, 0):
        for flip in (1, 0):
            if far or flip:
                peer = lax.rem(xh + flip, 2) * 8 + lax.rem(z + far, 8)
                pl.semaphore_signal(barrier, inc=1, device_id=(ax, peer, grp), device_id_type=MESH)
        for flip in range(4):
            if far or flip:
                peer = (2 * lax.rem(y + far, 8) + lax.rem(core + flip // 2, 2), th, lax.rem(grp + flip, 2))
                pl.semaphore_signal(barrier, inc=1, device_id=peer, device_id_type=MESH)

    halves = [ref.at[pl.ds(2 * ch, 2)] for ref in (fields_h, F) for ch in range(2)]
    sources = (*halves[:2], wall_h, fm_h, inv_h, wm_h, winv_h, ttab_h, xtab_h)
    targets = (*halves[2:], W, fm, inv, wm, winv, ttab, xtab)
    loads = [pltpu.make_async_copy(src, dst, ld.at[i]) for i, (src, dst) in enumerate(zip(sources, targets))]
    for load in loads:
        load.start()
    *load_f, load_w = loads[:3]
    load_rest = loads[3:]

    F2 = F.reshape(4 * XL * TL, R)

    def turn(ch):
        def step(t, _):
            for cc in range(2):
                fT[ch, 2 * t + cc] = F2[pl.ds((2 * ch + cc) * XL * TL + t, XL, stride=TL), :]
            return 0

        lax.fori_loop(0, TL, step, 0)
        swap_all(fT, ch)

    low = lax.broadcasted_iota(jnp.int32, (XL, R), 1) < RW

    def swap_halves(ref, ch, yy):
        at = 6 * yy + 2
        one, two = ref[ch, at], ref[ch, at + 1]
        ref[ch, at] = jnp.where(low, one, pltpu.roll(two, RW, axis=1))
        ref[ch, at + 1] = jnp.where(low, pltpu.roll(one, RW, axis=1), two)

    def swap_all(ref, ch):
        def step(yy, _):
            swap_halves(ref, ch, yy)
            return 0

        lax.fori_loop(0, 8, step, 0)

    def pair_walls():
        load_w.wait()
        for p in range(8):
            WP[p] = jnp.concatenate([W[p], W[p + 8]], axis=1)
        WP2 = WP.reshape(8 * TL, R)
        for t in range(TL):
            wT[t] = WP2[pl.ds(t, 8, stride=TL), :]

    def offset(i):
        return 4 + lax.div(i + 1, 2) * (1 - 2 * lax.rem(i, 2))

    def send(remote, src, dst, s_sem, r_sem, device):
        @pl.when(remote)
        def _():
            pltpu.make_async_remote_copy(
                src_ref=src, dst_ref=dst, send_sem=s_sem, recv_sem=r_sem, device_id=device, device_id_type=MESH
            ).start()

        @pl.when(jnp.logical_not(remote))
        def _():
            pltpu.make_async_copy(src, dst, r_sem).start()

    def theta_peer(i, flip):
        return lax.rem(xh + flip, 2) * 8 + lax.rem(z + offset(i), 8)

    def send_chunk(ch):
        load_f[ch].wait()
        if ch == 0:
            pl.semaphore_wait(barrier, NT - 1 + NA - 1)

        def step_t(i, _):
            for flip in (1, 0):
                t = theta_peer(i, flip)
                send(
                    t != th, F.at[pl.ds(2 * ch, 2), t], Qt.at[pl.ds(2 * ch, 2), pl.ds(TL * th, TL)],
                    sT.at[ch], rT.at[ch], (ax, t, grp),
                )
            return 0

        lax.fori_loop(0, 8, step_t, 0)
        turn(ch)

        def step(i, _):
            yy = lax.rem(y + offset(i), 8)
            for g_to in range(2):
                a_to = 4 * yy + g_to
                send(
                    a_to != a, fT.at[ch, pl.ds(6 * yy + 4 * g_to, 2)], Qx.at[pl.ds(2 * ch, 2), pl.ds(XL * a, XL)],
                    sX.at[ch], rX.at[ch], (2 * yy, th, g_to),
                )
                send(
                    a_to + 2 != a, fT.at[ch, 6 * yy + 2 + g_to], Qx.at[ch, pl.ds(XL * a, XL)],
                    sX.at[ch], rX.at[ch], (2 * yy + 1, th, g_to),
                )
            return 0

        lax.fori_loop(0, 8, step, 0)

    def send_wall():
        def step(i, _):
            p = lax.rem(z + offset(i), 8)
            t = lax.rem(p, 2) * 8 + p
            send(t != th, WP.at[p], Wt.at[pl.ds(TL * th, TL)], sWT, rWT, (ax, t, grp))
            yy = lax.rem(y + offset(i), 8)
            for g_to in range(2):
                slots = pl.ds(0, 2 - g_to)
                send(
                    4 * yy + 2 + g_to != a, wT.at[pl.ds(3 * yy + 2 * g_to, 2 - g_to)], Wx.at[slots, pl.ds(8 * a, 8)],
                    sWX, rWX, (2 * yy + 1, th, g_to),
                )
            return 0

        lax.fori_loop(0, 8, step, 0)

    send_chunk(0)
    pair_walls()
    send_wall()
    send_chunk(1)

    for load in load_rest:
        load.wait()
    lane = lax.broadcasted_iota(jnp.int32, (TL, R), 1)
    m = fm[...]
    row_r = -0.5 * ADVECT_R * m
    row_lift = COUPLE_T * m * m
    wm2 = jnp.concatenate([wm[...], wm[...]], axis=1)
    row_wlift = COUPLE_W * wm2 * wm2

    kk = lax.broadcasted_iota(jnp.int32, (R, R), 0)
    jj = lax.broadcasted_iota(jnp.int32, (R, R), 1)
    spread = 1.0 / m
    spread_t = jnp.broadcast_to(spread, (R, R)).T
    beyond = jnp.sum(jnp.where(kk >= jj, spread_t, 0.0), axis=0, keepdims=True)
    total = jnp.sum(spread_t, axis=0, keepdims=True)
    radius = 1.0 - 0.5 * (beyond - 0.5 * spread) / total
    row_t1 = -ADVECT_T / radius
    row_t2 = 1.0 / (radius * radius)
    wspread = 1.0 / wm2
    wspread_t = jnp.broadcast_to(wspread, (R, R)).T
    within = jnp.sum(jnp.where(kk <= lax.rem(jj, RW), wspread_t, 0.0), axis=0, keepdims=True)
    wtotal = jnp.sum(jnp.where(kk < RW, wspread_t, 0.0), axis=0, keepdims=True)
    wradius = 1.0 + 0.2 * (within - 0.5 * wspread) / wtotal
    row_w2 = LATERAL_W / (wradius * wradius)

    def prepare(p, _):
        pair = WP[p]
        for h in range(2):
            x = p + 8 * h
            u_r = F[2, x] * row_r
            ghost = pltpu.roll(pair, 127 - 64 * h, axis=1)
            for c in range(4):
                q = F[c, x]
                edge = ghost if c == 3 else 0.0
                upper = jnp.where(lane == R - 1, edge, pltpu.roll(q, R - 1, axis=1))
                lower = jnp.where(lane == 0, q, pltpu.roll(q, 1, axis=1))
                value = q + u_r * (upper - lower)
                if c == 3:
                    value = value + jnp.where(lane == R - 1, row_lift * ghost, 0.0)
                base[c, x] = value
        last_0 = pltpu.roll(F[3, p], 1, axis=1)
        last_1 = pltpu.roll(F[3, p + 8], 65, axis=1)
        wbase[p] = pair + jnp.where(
            lane == 0, row_wlift * last_0, jnp.where(lane == RW, row_wlift * last_1, 0.0)
        )
        return 0

    lax.fori_loop(0, 8, prepare, 0)
    for i in range(2):
        parts[i] = inverse_parts(inv[i])

    def full(ref, sem):
        pltpu.make_async_copy(ref, ref, sem).wait()

    half_t = THETA // 2
    half_x = X // 2

    def lam(ch, cc):
        return jnp.where(ch == 1, LATERAL_T, LATERAL_U) if cc == 1 else LATERAL_U

    def theta_chunk(ch):
        both = pl.ds(2 * ch, 2)
        full(Qt.at[both], rT.at[ch])
        top = jnp.concatenate([Qt[2 * ch, :half_t], Qt[2 * ch + 1, :half_t]], axis=1)
        bottom = jnp.concatenate([Qt[2 * ch, half_t:], Qt[2 * ch + 1, half_t:]], axis=1)
        firsts = apply_folded(ttab, slice(0, half_t), top, bottom)
        seconds = apply_folded(ttab, slice(half_t, THETA), top, bottom)
        for h in range(2):
            rows = slice(h * half_t, (h + 1) * half_t)
            swirl = Qt[1, rows] * row_t1
            for cc in range(2):
                cols = slice(cc * R, (cc + 1) * R)
                Rt[2 * ch + cc, rows] = swirl * firsts[h][:, cols] + seconds[h][:, cols] * (row_t2 * lam(ch, cc))

        def step(i, _):
            for flip in (1, 0):
                t = theta_peer(i, flip)
                send(
                    t != th, Rt.at[both, pl.ds(TL * t, TL)], cih.at[both, th], bsT.at[ch], brT.at[ch], (ax, t, grp)
                )
            return 0

        lax.fori_loop(0, 8, step, 0)

    def axial_chunk(ch):
        both = pl.ds(2 * ch, 2)
        full(Qx.at[both], rX.at[ch])
        top = jnp.concatenate([Qx[2 * ch, :half_x], Qx[2 * ch + 1, :half_x]], axis=1)
        bottom = jnp.concatenate([Qx[2 * ch, half_x:], Qx[2 * ch + 1, half_x:]], axis=1)
        firsts = apply_folded(xtab, slice(0, half_x), top, bottom)
        seconds = apply_folded(xtab, slice(half_x, X), top, bottom)
        for h in range(2):
            rows = slice(h * half_x, (h + 1) * half_x)
            stream = Qx[0, rows] * (-ADVECT_X)
            for cc in range(2):
                cols = slice(cc * R, (cc + 1) * R)
                Rx[2 * ch + cc, rows] = stream * firsts[h][:, cols] + seconds[h][:, cols] * lam(ch, cc)

        def step(i, _):
            yy = lax.rem(y + offset(i), 8)
            for k in range(4):
                a_to = 4 * yy + k
                send(
                    a_to != a, Rx.at[both, pl.ds(XL * a_to, XL)], axh.at[ch, pl.ds(2 * my_theta, 2)],
                    bsX.at[ch], brX.at[ch], (2 * yy + k // 2, th, k % 2),
                )
            return 0

        lax.fori_loop(0, 8, step, 0)

    lam_halves = jnp.where(lane[:1] < RW, LATERAL_U, LATERAL_T)

    def axial_half(ch):
        full(Qx.at[ch], rX.at[ch])
        firsts = apply_folded(xtab, slice(0, half_x), Qx[ch, :half_x], Qx[ch, half_x:])
        seconds = apply_folded(xtab, slice(half_x, X), Qx[ch, :half_x], Qx[ch, half_x:])
        lam_row = jnp.where(ch == 1, lam_halves, LATERAL_U)
        low_x = lax.broadcasted_iota(jnp.int32, (half_x, R), 1) < RW
        for h in range(2):
            rows = slice(h * half_x, (h + 1) * half_x)
            stream = Qx[0, rows] * (-ADVECT_X)
            stream = jnp.where(low_x, stream, pltpu.roll(stream, RW, axis=1))
            Rx[ch, rows] = stream * firsts[h] + seconds[h] * lam_row

        def step(i, _):
            yy = lax.rem(y + offset(i), 8)
            for k in range(4):
                a_to = 4 * yy + k
                send(
                    a_to != a, Rx.at[ch, pl.ds(XL * a_to, XL)], axh.at[ch, 6 * y + 2 + grp],
                    bsX.at[ch], brX.at[ch], (2 * yy + k // 2, th, k % 2),
                )
            return 0

        lax.fori_loop(0, 8, step, 0)

    def theta_wall():
        full(Wt, rWT)
        seconds = apply_folded(ttab, slice(half_t, THETA), Wt[:half_t], Wt[half_t:])
        for h in range(2):
            WRt[h * half_t:(h + 1) * half_t] = seconds[h] * row_w2

        def step(i, _):
            for flip in (1, 0):
                t = theta_peer(i, flip)
                send(t != th, WRt.at[pl.ds(TL * t, TL)], cwh.at[z], bsWT, brWT, (ax, t, grp))
            return 0

        lax.fori_loop(0, 8, step, 0)

    low8 = lax.broadcasted_iota(jnp.int32, (8, R), 1) < RW

    def axial_wall(g):
        slots = pl.ds(0, 2 - g)
        full(Wx.at[slots], rWX)

        def unpack(s, _):
            rows = pl.ds(pl.multiple_of(8 * s, 8), 8)
            even = pl.ds(pl.multiple_of(16 * s, 8), 8)
            odd = pl.ds(pl.multiple_of(16 * s + 8, 8), 8)
            w0 = Wx[0, rows]
            w1 = Wx[1 - g, rows]
            Wn[even] = jnp.where(low8, w0, pltpu.roll(w1, RW, axis=1))
            Wn[odd] = jnp.where(low8, pltpu.roll(w0, RW, axis=1), w1)
            return 0

        lax.fori_loop(0, NA, unpack, 0)
        seconds = apply_folded(xtab, slice(half_x, X), Wn[:half_x], Wn[half_x:])
        for h in range(2):
            Wn[h * half_x:(h + 1) * half_x] = seconds[h] * LATERAL_W

        def pack(s, _):
            rows = pl.ds(pl.multiple_of(8 * s, 8), 8)
            even = Wn[pl.ds(pl.multiple_of(16 * s, 8), 8)]
            odd = Wn[pl.ds(pl.multiple_of(16 * s + 8, 8), 8)]
            WRx[0, rows] = jnp.where(low8, even, pltpu.roll(odd, RW, axis=1))
            if g == 0:
                WRx[1, rows] = jnp.where(low8, pltpu.roll(even, RW, axis=1), odd)
            return 0

        lax.fori_loop(0, NA, pack, 0)

        def step(i, _):
            yy = lax.rem(y + offset(i), 8)
            for k in range(4):
                a_to = 4 * yy + k
                send(
                    a_to != a, WRx.at[slots, pl.ds(8 * a_to, 8)], awh.at[pl.ds(3 * y + 2 * g, 2 - g)],
                    bsWX, brWX, (2 * yy + k // 2, th, k % 2),
                )
            return 0

        lax.fori_loop(0, 8, step, 0)

    theta_chunk(0)
    pl.when(x_whole)(lambda: axial_chunk(0))
    pl.when(x_half)(lambda: axial_half(0))
    pl.when(jnp.logical_and(x_half, grp == 0))(lambda: axial_wall(0))
    pl.when(jnp.logical_and(x_half, grp == 1))(lambda: axial_wall(1))
    pl.when(t_wall)(theta_wall)
    theta_chunk(1)
    pl.when(x_whole)(lambda: axial_chunk(1))
    pl.when(x_half)(lambda: axial_half(1))

    axh2 = axh.reshape(4 * XL * TL, R)

    def gather(ch, out):
        full(cih.at[pl.ds(2 * ch, 2)], brT.at[ch])
        full(axh.at[ch], brX.at[ch])
        swap_all(axh, ch)

        def add(x, _):
            for cc in range(2):
                c = 2 * ch + cc
                axial = axh2[pl.ds(ch * 2 * XL * TL + cc * XL + x, TL, stride=2 * XL), :]
                out[cc, x] = base[c, x] + cih[c, x] + axial
            return 0

        lax.fori_loop(0, XL, add, 0)

    gather(0, done)
    for c in range(2):
        done[c] = apply_inverse(parts[0], done[c].reshape(XL * TL, R)).reshape(XL, TL, R)
    full(cwh, brWT)
    full(awh, brWX)
    awh2 = awh.reshape(8 * TL, R)

    def gather_wall(p, _):
        wbase[p] = wbase[p] + cwh[p] + awh2[pl.ds(p, TL, stride=8), :]
        return 0

    lax.fori_loop(0, 8, gather_wall, 0)
    value = wbase[...].reshape(8 * TL, R)
    nothing = jnp.zeros((RW, RW), F32)
    for h in range(2):
        pair = [winv[...], nothing] if h == 0 else [nothing, winv[...]]
        matrix = inverse_parts(jnp.concatenate(pair, axis=1))
        wdone[8 * h:8 * h + 8] = apply_inverse(matrix, value).reshape(8, TL, RW)
    gather(1, rest)

    for ch in range(2):
        full(F.at[pl.ds(0, 2), pl.ds(0, NT - 1)], sT.at[ch])
        full(F.at[pl.ds(0, 2), pl.ds(0, NT - 1)], bsT.at[ch])

        @pl.when(x_whole)
        def _():
            full(fT.at[ch, pl.ds(0, 2 * TL - 2)], sX.at[ch])
            full(Rx.at[pl.ds(0, 2), pl.ds(0, X - XL)], bsX.at[ch])

        @pl.when(x_half)
        def _():
            full(fT.at[ch, pl.ds(0, 2 * TL - 1)], sX.at[ch])
            full(Rx.at[0, pl.ds(0, X - XL)], bsX.at[ch])

    @pl.when(t_wall)
    def _():
        full(WP.at[pl.ds(0, 7)], sWT)
        full(WRt.at[pl.ds(0, THETA - TL)], bsWT)

    @pl.when(jnp.logical_not(t_wall))
    def _():
        full(WP, sWT)

    @pl.when(x_whole)
    def _():
        full(wT, sWX)

    for g in range(2):
        @pl.when(jnp.logical_and(x_half, grp == g))
        def _():
            full(wT.at[pl.ds(0, TL - 2 + g)], sWX)
            full(WRx.at[pl.ds(0, 2 - g), pl.ds(0, 8 * (NA - 1))], bsWX)


def last_kernel(done, rest, wdone, parts, out_h, wout_h, buf, st):
    copies = [
        pltpu.make_async_copy(done, out_h.at[pl.ds(0, 2)], st.at[0]),
        pltpu.make_async_copy(wdone, wout_h, st.at[1]),
    ]
    for copy in copies:
        copy.start()
    for c in range(2):
        buf[c] = apply_inverse(parts[c], rest[c].reshape(XL * TL, R)).reshape(XL, TL, R)
        copy = pltpu.make_async_copy(buf.at[c], out_h.at[2 + c], st.at[2 + c])
        copy.start()
        copies.append(copy)
    for copy in copies:
        copy.wait()


def shards(fields, wall_temp, fluid_metric, fluid_radial_inverses, wall_metric, wall_inverse):
    vmem = pl.BlockSpec(memory_space=pltpu.VMEM)
    hbm = pl.BlockSpec(memory_space=pltpu.HBM)
    dma = pltpu.SemaphoreType.DMA
    ttab = jnp.asarray(folded_tables(THETA))
    xtab = jnp.asarray(folded_tables(X))

    def buf(*shape, dtype=F32):
        return pltpu.VMEM(shape, dtype)

    done, rest, wdone, parts = pl.pallas_call(
        kernel,
        out_shape=(buf(2, XL, TL, R), buf(2, XL, TL, R), buf(XL, TL, RW), buf(2, R, 3 * R, dtype=BF16)),
        in_specs=[hbm] * 8,
        out_specs=(vmem,) * 4,
        scratch_shapes=[
            buf(4, XL, TL, R), buf(XL, TL, RW), buf(1, R), buf(2, R, R), buf(1, RW), buf(RW, RW),
            buf(*ttab.shape, dtype=BF16), buf(*xtab.shape, dtype=BF16),
            buf(2, 2 * TL, XL, R), buf(8, TL, R), buf(TL, 8, R),
            buf(4, THETA, R), buf(4, X, R), buf(THETA, R), buf(2, X // 2, R),
            buf(4, THETA, R), buf(4, X, R), buf(THETA, R), buf(2, X // 2, R), buf(X, R),
            buf(4, XL, TL, R), buf(2, 2 * TL, XL, R), buf(8, TL, R), buf(TL, 8, R),
            buf(4, XL, TL, R), buf(8, TL, R),
            dma((9,)),
            dma((2,)), dma((2,)), dma((2,)), dma((2,)), dma, dma, dma, dma,
            dma((2,)), dma((2,)), dma((2,)), dma((2,)), dma, dma, dma, dma,
        ],
        compiler_params=pltpu.CompilerParams(
            collective_id=0, has_side_effects=True, vmem_limit_bytes=64128 * 2**10
        ),
    )(
        fields, wall_temp, fluid_metric.reshape(1, R), fluid_radial_inverses,
        wall_metric.reshape(1, RW), wall_inverse, ttab, xtab,
    )
    return pl.pallas_call(
        last_kernel,
        out_shape=(
            jax.ShapeDtypeStruct((4, XL, TL, R), F32),
            jax.ShapeDtypeStruct((XL, TL, RW), F32),
        ),
        in_specs=[vmem] * 4,
        out_specs=(hbm, hbm),
        scratch_shapes=[buf(2, XL, TL, R), dma((4,))],
        compiler_params=pltpu.CompilerParams(vmem_limit_bytes=16 * 2**20),
    )(done, rest, wdone, parts)


def solution(mesh):
    in_specs = (
        P(None, ("ax", "grp"), "th", None),
        P(("ax", "grp"), "th", None),
        P(),
        P(),
        P(),
        P(),
    )
    out_specs = (P(None, ("ax", "grp"), "th", None), P(("ax", "grp"), "th", None))
    return jax.shard_map(shards, mesh=mesh, in_specs=in_specs, out_specs=out_specs, check_vma=False)
```

```python
import functools

import jax
import jax.numpy as jnp
import numpy as np
from jax import lax
from jax.experimental import pallas as pl
from jax.experimental.pallas import tpu as pltpu
from jax.sharding import PartitionSpec as P

MESH = pl.DeviceIdType.MESH
F32 = jnp.float32
BF16 = jnp.bfloat16

X = 512
THETA = 384
R = 128
RW = 64
XL = 16
TL = 24
NT = 16
NA = 32

ADVECT_X = 0.08
ADVECT_T = 0.08
ADVECT_R = 0.15
LATERAL_U = 0.03
LATERAL_T = 0.04
LATERAL_W = 0.1
COUPLE_T = 0.6
COUPLE_W = 0.8


def folded_tables(points):
    spacing = 2.0 * np.pi / points
    offset = np.arange(points)[:, None] - np.arange(points)[None, :]
    parity = 1.0 - 2.0 * (offset % 2)
    angle = np.where(offset != 0, offset * 0.5 * spacing, 1.0)
    first = np.where(offset != 0, 0.5 * spacing * parity / np.tan(angle), 0.0)
    second = np.where(
        offset != 0,
        -parity * spacing**2 / (2.0 * np.sin(angle) ** 2),
        -(np.pi**2 / 3.0 + spacing**2 / 6.0),
    )
    half = points // 2
    parts = []
    for sign in (1.0, -1.0):
        both = np.concatenate(
            [0.5 * (table[:half, :half] + sign * table[:half, half:]) for table in (first, second)], axis=0
        ).astype(np.float32)
        high = both.astype(BF16)
        low = (both - high.astype(np.float32)).astype(BF16)
        parts.append(np.stack([high, low]))
    return np.stack(parts)


def split(value):
    high = value.astype(BF16)
    low = (value - high.astype(F32)).astype(BF16)
    return high, low


def dot(a, b):
    return jnp.dot(a, b, preferred_element_type=F32)


def dot_t(a, b):
    return lax.dot_general(a, b, (((1,), (1,)), ((), ())), preferred_element_type=F32)


def inverse_parts(matrix):
    high, low = split(matrix)
    return jnp.concatenate([high, high, low], axis=1)


def apply_inverse(parts, value):
    high, low = split(value)
    return dot_t(jnp.concatenate([high, low, high], axis=1), parts)


def apply_folded(table, rows, top, bottom):
    results = []
    for which, value in ((0, top + bottom), (1, top - bottom)):
        high, low = split(value)
        t_high = table[which, 0, rows, :]
        t_low = table[which, 1, rows, :]
        results.append(dot(t_high, high) + dot(t_high, low) + dot(t_low, high))
    return results[0] + results[1], results[0] - results[1]


def kernel(
    fields_h, wall_h, fm_h, inv_h, wm_h, winv_h, ttab_h, xtab_h,
    done, rest, wdone, parts,
    F, W, fm, inv, wm, winv, ttab, xtab,
    fT, WP, wT,
    Qt, Qx, Wt, Wx,
    Rt, Rx, WRt, WRx, Wn,
    cih, axh, cwh, awh,
    base, wbase,
    ld,
    sT, rT, sX, rX, sWT, rWT, sWX, rWX,
    bsT, brT, bsX, brX, bsWT, brWT, bsWX, brWX,
):
    ax = lax.axis_index("ax")
    th = lax.axis_index("th")
    grp = lax.axis_index("grp")
    a = ax * 2 + grp
    y = lax.div(ax, 2)
    core = lax.rem(ax, 2)
    xh = lax.div(th, 8)
    z = lax.rem(th, 8)
    x_whole = core == 0
    x_half = core == 1
    my_theta = 3 * y + 2 * grp
    t_wall = xh == lax.rem(z, 2)

    barrier = pltpu.get_barrier_semaphore()

    for far in (4, 3, 5, 2, 6, 1, 7, 0):
        for flip in (1, 0):
            if far or flip:
                peer = lax.rem(xh + flip, 2) * 8 + lax.rem(z + far, 8)
                pl.semaphore_signal(barrier, inc=1, device_id=(ax, peer, grp), device_id_type=MESH)
        for flip in range(4):
            if far or flip:
                peer = (2 * lax.rem(y + far, 8) + lax.rem(core + flip // 2, 2), th, lax.rem(grp + flip, 2))
                pl.semaphore_signal(barrier, inc=1, device_id=peer, device_id_type=MESH)

    halves = [ref.at[pl.ds(2 * ch, 2)] for ref in (fields_h, F) for ch in range(2)]
    sources = (*halves[:2], wall_h, fm_h, inv_h, wm_h, winv_h, ttab_h, xtab_h)
    targets = (*halves[2:], W, fm, inv, wm, winv, ttab, xtab)
    loads = [pltpu.make_async_copy(src, dst, ld.at[i]) for i, (src, dst) in enumerate(zip(sources, targets))]
    for load in loads:
        load.start()
    *load_f, load_w = loads[:3]
    load_rest = loads[3:]

    F2 = F.reshape(4 * XL * TL, R)

    def turn(ch):
        def step(group, _):
            for i in range(4):
                t = 4 * group + i
                for cc in range(2):
                    fT[ch, 2 * t + cc] = F2[pl.ds((2 * ch + cc) * XL * TL + t, XL, stride=TL), :]
            return 0

        lax.fori_loop(0, TL // 4, step, 0)
        swap_all(fT, ch)

    low = lax.broadcasted_iota(jnp.int32, (XL, R), 1) < RW

    def swap_halves(ref, ch, yy):
        at = 6 * yy + 2
        one, two = ref[ch, at], ref[ch, at + 1]
        ref[ch, at] = jnp.where(low, one, pltpu.roll(two, RW, axis=1))
        ref[ch, at + 1] = jnp.where(low, pltpu.roll(one, RW, axis=1), two)

    def swap_all(ref, ch):
        def step(group, _):
            for i in range(4):
                swap_halves(ref, ch, 4 * group + i)
            return 0

        lax.fori_loop(0, 2, step, 0)

    def pair_walls():
        load_w.wait()
        for p in range(8):
            WP[p] = jnp.concatenate([W[p], W[p + 8]], axis=1)
        WP2 = WP.reshape(8 * TL, R)
        for t in range(TL):
            wT[t] = WP2[pl.ds(t, 8, stride=TL), :]

    def offset(i):
        return 4 + lax.div(i + 1, 2) * (1 - 2 * lax.rem(i, 2))

    def send(remote, src, dst, s_sem, r_sem, device):
        @pl.when(remote)
        def _():
            pltpu.make_async_remote_copy(
                src_ref=src, dst_ref=dst, send_sem=s_sem, recv_sem=r_sem, device_id=device, device_id_type=MESH
            ).start()

        @pl.when(jnp.logical_not(remote))
        def _():
            pltpu.make_async_copy(src, dst, r_sem).start()

    def theta_peer(i, flip):
        return lax.rem(xh + flip, 2) * 8 + lax.rem(z + offset(i), 8)

    def send_chunk(ch):
        load_f[ch].wait()
        turn(ch)
        if ch == 0:
            pl.semaphore_wait(barrier, NT - 1 + NA - 1)

        def step(i, _):
            for flip in (1, 0):
                t = theta_peer(i, flip)
                send(
                    t != th, F.at[pl.ds(2 * ch, 2), t], Qt.at[pl.ds(2 * ch, 2), pl.ds(TL * th, TL)],
                    sT.at[ch], rT.at[ch], (ax, t, grp),
                )
            yy = lax.rem(y + offset(i), 8)
            for g_to in range(2):
                a_to = 4 * yy + g_to
                send(
                    a_to != a, fT.at[ch, pl.ds(6 * yy + 4 * g_to, 2)], Qx.at[pl.ds(2 * ch, 2), pl.ds(XL * a, XL)],
                    sX.at[ch], rX.at[ch], (2 * yy, th, g_to),
                )
                send(
                    a_to + 2 != a, fT.at[ch, 6 * yy + 2 + g_to], Qx.at[ch, pl.ds(XL * a, XL)],
                    sX.at[ch], rX.at[ch], (2 * yy + 1, th, g_to),
                )
            return 0

        lax.fori_loop(0, 8, step, 0)

    def send_wall():
        def step(i, _):
            p = lax.rem(z + offset(i), 8)
            t = lax.rem(p, 2) * 8 + p
            send(t != th, WP.at[p], Wt.at[pl.ds(TL * th, TL)], sWT, rWT, (ax, t, grp))
            yy = lax.rem(y + offset(i), 8)
            for g_to in range(2):
                slots = pl.ds(0, 2 - g_to)
                send(
                    4 * yy + 2 + g_to != a, wT.at[pl.ds(3 * yy + 2 * g_to, 2 - g_to)], Wx.at[slots, pl.ds(8 * a, 8)],
                    sWX, rWX, (2 * yy + 1, th, g_to),
                )
            return 0

        lax.fori_loop(0, 8, step, 0)

    send_chunk(0)
    pair_walls()
    send_wall()
    send_chunk(1)

    for load in load_rest:
        load.wait()
    lane = lax.broadcasted_iota(jnp.int32, (TL, R), 1)
    m = fm[...]
    row_r = -0.5 * ADVECT_R * m
    row_lift = COUPLE_T * m * m
    wm2 = jnp.concatenate([wm[...], wm[...]], axis=1)
    row_wlift = COUPLE_W * wm2 * wm2

    kk = lax.broadcasted_iota(jnp.int32, (R, R), 0)
    jj = lax.broadcasted_iota(jnp.int32, (R, R), 1)
    spread = 1.0 / m
    spread_t = jnp.broadcast_to(spread, (R, R)).T
    beyond = jnp.sum(jnp.where(kk >= jj, spread_t, 0.0), axis=0, keepdims=True)
    total = jnp.sum(spread_t, axis=0, keepdims=True)
    radius = 1.0 - 0.5 * (beyond - 0.5 * spread) / total
    row_t1 = -ADVECT_T / radius
    row_t2 = 1.0 / (radius * radius)
    wspread = 1.0 / wm2
    wspread_t = jnp.broadcast_to(wspread, (R, R)).T
    within = jnp.sum(jnp.where(kk <= lax.rem(jj, RW), wspread_t, 0.0), axis=0, keepdims=True)
    wtotal = jnp.sum(jnp.where(kk < RW, wspread_t, 0.0), axis=0, keepdims=True)
    wradius = 1.0 + 0.2 * (within - 0.5 * wspread) / wtotal
    row_w2 = LATERAL_W / (wradius * wradius)

    def prepare(p, _):
        pair = WP[p]
        for h in range(2):
            x = p + 8 * h
            u_r = F[2, x] * row_r
            ghost = pltpu.roll(pair, 127 - 64 * h, axis=1)
            for c in range(4):
                q = F[c, x]
                edge = ghost if c == 3 else 0.0
                upper = jnp.where(lane == R - 1, edge, pltpu.roll(q, R - 1, axis=1))
                lower = jnp.where(lane == 0, q, pltpu.roll(q, 1, axis=1))
                value = q + u_r * (upper - lower)
                if c == 3:
                    value = value + jnp.where(lane == R - 1, row_lift * ghost, 0.0)
                base[c, x] = value
        last_0 = pltpu.roll(F[3, p], 1, axis=1)
        last_1 = pltpu.roll(F[3, p + 8], 65, axis=1)
        wbase[p] = pair + jnp.where(
            lane == 0, row_wlift * last_0, jnp.where(lane == RW, row_wlift * last_1, 0.0)
        )
        return 0

    lax.fori_loop(0, 8, prepare, 0)
    for i in range(2):
        parts[i] = inverse_parts(inv[i])

    def full(ref, sem):
        pltpu.make_async_copy(ref, ref, sem).wait()

    half_t = THETA // 2
    half_x = X // 2

    def lam(ch, cc):
        return jnp.where(ch == 1, LATERAL_T, LATERAL_U) if cc == 1 else LATERAL_U

    def theta_chunk(ch):
        both = pl.ds(2 * ch, 2)
        full(Qt.at[both], rT.at[ch])
        top = jnp.concatenate([Qt[2 * ch, :half_t], Qt[2 * ch + 1, :half_t]], axis=1)
        bottom = jnp.concatenate([Qt[2 * ch, half_t:], Qt[2 * ch + 1, half_t:]], axis=1)
        firsts = apply_folded(ttab, slice(0, half_t), top, bottom)
        seconds = apply_folded(ttab, slice(half_t, THETA), top, bottom)
        for h in range(2):
            rows = slice(h * half_t, (h + 1) * half_t)
            swirl = Qt[1, rows] * row_t1
            for cc in range(2):
                cols = slice(cc * R, (cc + 1) * R)
                Rt[2 * ch + cc, rows] = swirl * firsts[h][:, cols] + seconds[h][:, cols] * (row_t2 * lam(ch, cc))

        def step(i, _):
            for flip in (1, 0):
                t = theta_peer(i, flip)
                send(
                    t != th, Rt.at[both, pl.ds(TL * t, TL)], cih.at[both, th], bsT.at[ch], brT.at[ch], (ax, t, grp)
                )
            return 0

        lax.fori_loop(0, 8, step, 0)

    def axial_chunk(ch):
        both = pl.ds(2 * ch, 2)
        full(Qx.at[both], rX.at[ch])
        top = jnp.concatenate([Qx[2 * ch, :half_x], Qx[2 * ch + 1, :half_x]], axis=1)
        bottom = jnp.concatenate([Qx[2 * ch, half_x:], Qx[2 * ch + 1, half_x:]], axis=1)
        firsts = apply_folded(xtab, slice(0, half_x), top, bottom)
        seconds = apply_folded(xtab, slice(half_x, X), top, bottom)
        for h in range(2):
            rows = slice(h * half_x, (h + 1) * half_x)
            stream = Qx[0, rows] * (-ADVECT_X)
            for cc in range(2):
                cols = slice(cc * R, (cc + 1) * R)
                Rx[2 * ch + cc, rows] = stream * firsts[h][:, cols] + seconds[h][:, cols] * lam(ch, cc)

        def step(i, _):
            yy = lax.rem(y + offset(i), 8)
            for k in range(4):
                a_to = 4 * yy + k
                send(
                    a_to != a, Rx.at[both, pl.ds(XL * a_to, XL)], axh.at[ch, pl.ds(2 * my_theta, 2)],
                    bsX.at[ch], brX.at[ch], (2 * yy + k // 2, th, k % 2),
                )
            return 0

        lax.fori_loop(0, 8, step, 0)

    lam_halves = jnp.where(lane[:1] < RW, LATERAL_U, LATERAL_T)

    def axial_half(ch):
        full(Qx.at[ch], rX.at[ch])
        firsts = apply_folded(xtab, slice(0, half_x), Qx[ch, :half_x], Qx[ch, half_x:])
        seconds = apply_folded(xtab, slice(half_x, X), Qx[ch, :half_x], Qx[ch, half_x:])
        lam_row = jnp.where(ch == 1, lam_halves, LATERAL_U)
        low_x = lax.broadcasted_iota(jnp.int32, (half_x, R), 1) < RW
        for h in range(2):
            rows = slice(h * half_x, (h + 1) * half_x)
            stream = Qx[0, rows] * (-ADVECT_X)
            stream = jnp.where(low_x, stream, pltpu.roll(stream, RW, axis=1))
            Rx[ch, rows] = stream * firsts[h] + seconds[h] * lam_row

        def step(i, _):
            yy = lax.rem(y + offset(i), 8)
            for k in range(4):
                a_to = 4 * yy + k
                send(
                    a_to != a, Rx.at[ch, pl.ds(XL * a_to, XL)], axh.at[ch, 6 * y + 2 + grp],
                    bsX.at[ch], brX.at[ch], (2 * yy + k // 2, th, k % 2),
                )
            return 0

        lax.fori_loop(0, 8, step, 0)

    def theta_wall():
        full(Wt, rWT)
        seconds = apply_folded(ttab, slice(half_t, THETA), Wt[:half_t], Wt[half_t:])
        for h in range(2):
            WRt[h * half_t:(h + 1) * half_t] = seconds[h] * row_w2

        def step(i, _):
            for flip in (1, 0):
                t = theta_peer(i, flip)
                send(t != th, WRt.at[pl.ds(TL * t, TL)], cwh.at[z], bsWT, brWT, (ax, t, grp))
            return 0

        lax.fori_loop(0, 8, step, 0)

    low8 = lax.broadcasted_iota(jnp.int32, (8, R), 1) < RW

    def axial_wall(g):
        slots = pl.ds(0, 2 - g)
        full(Wx.at[slots], rWX)

        def unpack(s, _):
            rows = pl.ds(pl.multiple_of(8 * s, 8), 8)
            even = pl.ds(pl.multiple_of(16 * s, 8), 8)
            odd = pl.ds(pl.multiple_of(16 * s + 8, 8), 8)
            w0 = Wx[0, rows]
            w1 = Wx[1 - g, rows]
            Wn[even] = jnp.where(low8, w0, pltpu.roll(w1, RW, axis=1))
            Wn[odd] = jnp.where(low8, pltpu.roll(w0, RW, axis=1), w1)
            return 0

        lax.fori_loop(0, NA, unpack, 0)
        seconds = apply_folded(xtab, slice(half_x, X), Wn[:half_x], Wn[half_x:])
        for h in range(2):
            Wn[h * half_x:(h + 1) * half_x] = seconds[h] * LATERAL_W

        def pack(s, _):
            rows = pl.ds(pl.multiple_of(8 * s, 8), 8)
            even = Wn[pl.ds(pl.multiple_of(16 * s, 8), 8)]
            odd = Wn[pl.ds(pl.multiple_of(16 * s + 8, 8), 8)]
            WRx[0, rows] = jnp.where(low8, even, pltpu.roll(odd, RW, axis=1))
            if g == 0:
                WRx[1, rows] = jnp.where(low8, pltpu.roll(even, RW, axis=1), odd)
            return 0

        lax.fori_loop(0, NA, pack, 0)

        def step(i, _):
            yy = lax.rem(y + offset(i), 8)
            for k in range(4):
                a_to = 4 * yy + k
                send(
                    a_to != a, WRx.at[slots, pl.ds(8 * a_to, 8)], awh.at[pl.ds(3 * y + 2 * g, 2 - g)],
                    bsWX, brWX, (2 * yy + k // 2, th, k % 2),
                )
            return 0

        lax.fori_loop(0, 8, step, 0)

    theta_chunk(0)
    pl.when(x_whole)(lambda: axial_chunk(0))
    pl.when(x_half)(lambda: axial_half(0))
    pl.when(jnp.logical_and(x_half, grp == 0))(lambda: axial_wall(0))
    pl.when(jnp.logical_and(x_half, grp == 1))(lambda: axial_wall(1))
    pl.when(t_wall)(theta_wall)
    theta_chunk(1)
    pl.when(x_whole)(lambda: axial_chunk(1))
    pl.when(x_half)(lambda: axial_half(1))

    axh2 = axh.reshape(4 * XL * TL, R)

    def gather(ch, out):
        full(cih.at[pl.ds(2 * ch, 2)], brT.at[ch])
        full(axh.at[ch], brX.at[ch])
        swap_all(axh, ch)

        def add(group, _):
            for i in range(4):
                x = 4 * group + i
                for cc in range(2):
                    c = 2 * ch + cc
                    axial = axh2[pl.ds(ch * 2 * XL * TL + cc * XL + x, TL, stride=2 * XL), :]
                    out[cc, x] = base[c, x] + cih[c, x] + axial
            return 0

        lax.fori_loop(0, XL // 4, add, 0)

    gather(0, done)
    for c in range(2):
        done[c] = apply_inverse(parts[0], done[c].reshape(XL * TL, R)).reshape(XL, TL, R)
    full(cwh, brWT)
    full(awh, brWX)
    awh2 = awh.reshape(8 * TL, R)

    def gather_wall(p, _):
        wbase[p] = wbase[p] + cwh[p] + awh2[pl.ds(p, TL, stride=8), :]
        return 0

    lax.fori_loop(0, 8, gather_wall, 0)
    value = wbase[...].reshape(8 * TL, R)
    nothing = jnp.zeros((RW, RW), F32)
    for h in range(2):
        pair = [winv[...], nothing] if h == 0 else [nothing, winv[...]]
        matrix = inverse_parts(jnp.concatenate(pair, axis=1))
        wdone[8 * h:8 * h + 8] = apply_inverse(matrix, value).reshape(8, TL, RW)
    gather(1, rest)

    for ch in range(2):
        full(F.at[pl.ds(0, 2), pl.ds(0, NT - 1)], sT.at[ch])
        full(F.at[pl.ds(0, 2), pl.ds(0, NT - 1)], bsT.at[ch])

        @pl.when(x_whole)
        def _():
            full(fT.at[ch, pl.ds(0, 2 * TL - 2)], sX.at[ch])
            full(Rx.at[pl.ds(0, 2), pl.ds(0, X - XL)], bsX.at[ch])

        @pl.when(x_half)
        def _():
            full(fT.at[ch, pl.ds(0, 2 * TL - 1)], sX.at[ch])
            full(Rx.at[0, pl.ds(0, X - XL)], bsX.at[ch])

    @pl.when(t_wall)
    def _():
        full(WP.at[pl.ds(0, 7)], sWT)
        full(WRt.at[pl.ds(0, THETA - TL)], bsWT)

    @pl.when(jnp.logical_not(t_wall))
    def _():
        full(WP, sWT)

    @pl.when(x_whole)
    def _():
        full(wT, sWX)

    for g in range(2):
        @pl.when(jnp.logical_and(x_half, grp == g))
        def _():
            full(wT.at[pl.ds(0, TL - 2 + g)], sWX)
            full(WRx.at[pl.ds(0, 2 - g), pl.ds(0, 8 * (NA - 1))], bsWX)


def last_kernel(done, rest, wdone, parts, out_h, wout_h, buf, st):
    copies = [
        pltpu.make_async_copy(done, out_h.at[pl.ds(0, 2)], st.at[0]),
        pltpu.make_async_copy(wdone, wout_h, st.at[1]),
    ]
    for copy in copies:
        copy.start()
    for c in range(2):
        buf[c] = apply_inverse(parts[c], rest[c].reshape(XL * TL, R)).reshape(XL, TL, R)
        copy = pltpu.make_async_copy(buf.at[c], out_h.at[2 + c], st.at[2 + c])
        copy.start()
        copies.append(copy)
    for copy in copies:
        copy.wait()


def shards(fields, wall_temp, fluid_metric, fluid_radial_inverses, wall_metric, wall_inverse):
    vmem = pl.BlockSpec(memory_space=pltpu.VMEM)
    hbm = pl.BlockSpec(memory_space=pltpu.HBM)
    dma = pltpu.SemaphoreType.DMA
    ttab = jnp.asarray(folded_tables(THETA))
    xtab = jnp.asarray(folded_tables(X))

    def buf(*shape, dtype=F32):
        return pltpu.VMEM(shape, dtype)

    done, rest, wdone, parts = pl.pallas_call(
        kernel,
        out_shape=(buf(2, XL, TL, R), buf(2, XL, TL, R), buf(XL, TL, RW), buf(2, R, 3 * R, dtype=BF16)),
        in_specs=[hbm] * 8,
        out_specs=(vmem,) * 4,
        scratch_shapes=[
            buf(4, XL, TL, R), buf(XL, TL, RW), buf(1, R), buf(2, R, R), buf(1, RW), buf(RW, RW),
            buf(*ttab.shape, dtype=BF16), buf(*xtab.shape, dtype=BF16),
            buf(2, 2 * TL, XL, R), buf(8, TL, R), buf(TL, 8, R),
            buf(4, THETA, R), buf(4, X, R), buf(THETA, R), buf(2, X // 2, R),
            buf(4, THETA, R), buf(4, X, R), buf(THETA, R), buf(2, X // 2, R), buf(X, R),
            buf(4, XL, TL, R), buf(2, 2 * TL, XL, R), buf(8, TL, R), buf(TL, 8, R),
            buf(4, XL, TL, R), buf(8, TL, R),
            dma((9,)),
            dma((2,)), dma((2,)), dma((2,)), dma((2,)), dma, dma, dma, dma,
            dma((2,)), dma((2,)), dma((2,)), dma((2,)), dma, dma, dma, dma,
        ],
        compiler_params=pltpu.CompilerParams(
            collective_id=0, has_side_effects=True, vmem_limit_bytes=64128 * 2**10
        ),
    )(
        fields, wall_temp, fluid_metric.reshape(1, R), fluid_radial_inverses,
        wall_metric.reshape(1, RW), wall_inverse, ttab, xtab,
    )
    return pl.pallas_call(
        last_kernel,
        out_shape=(
            jax.ShapeDtypeStruct((4, XL, TL, R), F32),
            jax.ShapeDtypeStruct((XL, TL, RW), F32),
        ),
        in_specs=[vmem] * 4,
        out_specs=(hbm, hbm),
        scratch_shapes=[buf(2, XL, TL, R), dma((4,))],
        compiler_params=pltpu.CompilerParams(vmem_limit_bytes=16 * 2**20),
    )(done, rest, wdone, parts)


def solution(mesh):
    in_specs = (
        P(None, ("ax", "grp"), "th", None),
        P(("ax", "grp"), "th", None),
        P(),
        P(),
        P(),
        P(),
    )
    out_specs = (P(None, ("ax", "grp"), "th", None), P(("ax", "grp"), "th", None))
    return jax.shard_map(shards, mesh=mesh, in_specs=in_specs, out_specs=out_specs, check_vma=False)
```

```python
import functools

import jax
import jax.numpy as jnp
import numpy as np
from jax import lax
from jax.experimental import pallas as pl
from jax.experimental.pallas import tpu as pltpu
from jax.sharding import PartitionSpec as P

MESH = pl.DeviceIdType.MESH
F32 = jnp.float32
BF16 = jnp.bfloat16

X = 512
THETA = 384
R = 128
RW = 64
XL = 16
TL = 24
NT = 16
NA = 32

ADVECT_X = 0.08
ADVECT_T = 0.08
ADVECT_R = 0.15
LATERAL_U = 0.03
LATERAL_T = 0.04
LATERAL_W = 0.1
COUPLE_T = 0.6
COUPLE_W = 0.8


def folded_tables(points):
    spacing = 2.0 * np.pi / points
    offset = np.arange(points)[:, None] - np.arange(points)[None, :]
    parity = 1.0 - 2.0 * (offset % 2)
    angle = np.where(offset != 0, offset * 0.5 * spacing, 1.0)
    first = np.where(offset != 0, 0.5 * spacing * parity / np.tan(angle), 0.0)
    second = np.where(
        offset != 0,
        -parity * spacing**2 / (2.0 * np.sin(angle) ** 2),
        -(np.pi**2 / 3.0 + spacing**2 / 6.0),
    )
    half = points // 2
    parts = []
    for sign in (1.0, -1.0):
        both = np.concatenate(
            [0.5 * (table[:half, :half] + sign * table[:half, half:]) for table in (first, second)], axis=0
        ).astype(np.float32)
        high = both.astype(BF16)
        low = (both - high.astype(np.float32)).astype(BF16)
        parts.append(np.stack([high, low]))
    return np.stack(parts)


def split(value):
    high = value.astype(BF16)
    low = (value - high.astype(F32)).astype(BF16)
    return high, low


def dot(a, b):
    return jnp.dot(a, b, preferred_element_type=F32)


def dot_t(a, b):
    return lax.dot_general(a, b, (((1,), (1,)), ((), ())), preferred_element_type=F32)


def inverse_parts(matrix):
    high, low = split(matrix)
    return jnp.concatenate([high, high, low], axis=1)


def apply_inverse(parts, value):
    high, low = split(value)
    return dot_t(jnp.concatenate([high, low, high], axis=1), parts)


def apply_folded(table, rows, top, bottom):
    results = []
    for which, value in ((0, top + bottom), (1, top - bottom)):
        high, low = split(value)
        t_high = table[which, 0, rows, :]
        t_low = table[which, 1, rows, :]
        results.append(dot(t_high, high) + dot(t_high, low) + dot(t_low, high))
    return results[0] + results[1], results[0] - results[1]


def kernel(
    fields_h, wall_h, fm_h, inv_h, wm_h, winv_h, ttab_h, xtab_h,
    done, rest, wdone, parts,
    F, W, fm, inv, wm, winv, ttab, xtab,
    fT, WP, wT,
    Qt, Qx, Wt, Wx,
    Rt, Rx, WRt, WRx, Wn,
    cih, axh, cwh, awh,
    base, wbase,
    ld,
    sT, rT, sX, rX, sWT, rWT, sWX, rWX,
    bsT, brT, bsX, brX, bsWT, brWT, bsWX, brWX,
):
    ax = lax.axis_index("ax")
    th = lax.axis_index("th")
    grp = lax.axis_index("grp")
    a = ax * 2 + grp
    y = lax.div(ax, 2)
    core = lax.rem(ax, 2)
    xh = lax.div(th, 8)
    z = lax.rem(th, 8)
    x_whole = core == 0
    x_half = core == 1
    my_theta = 3 * y + 2 * grp
    t_wall = xh == lax.rem(z, 2)

    barrier = pltpu.get_barrier_semaphore()

    for far in (4, 3, 5, 2, 6, 1, 7, 0):
        for flip in (1, 0):
            if far or flip:
                peer = lax.rem(xh + flip, 2) * 8 + lax.rem(z + far, 8)
                pl.semaphore_signal(barrier, inc=1, device_id=(ax, peer, grp), device_id_type=MESH)
        for flip in range(4):
            if far or flip:
                peer = (2 * lax.rem(y + far, 8) + lax.rem(core + flip // 2, 2), th, lax.rem(grp + flip, 2))
                pl.semaphore_signal(barrier, inc=1, device_id=peer, device_id_type=MESH)

    halves = [ref.at[pl.ds(2 * ch, 2)] for ref in (fields_h, F) for ch in range(2)]
    sources = (*halves[:2], wall_h, fm_h, inv_h, wm_h, winv_h, ttab_h, xtab_h)
    targets = (*halves[2:], W, fm, inv, wm, winv, ttab, xtab)
    loads = [pltpu.make_async_copy(src, dst, ld.at[i]) for i, (src, dst) in enumerate(zip(sources, targets))]
    for load in loads:
        load.start()
    *load_f, load_w = loads[:3]
    load_rest = loads[3:]

    F2 = F.reshape(4 * XL * TL, R)

    def turn(ch):
        def step(group, _):
            for i in range(4):
                t = 4 * group + i
                for cc in range(2):
                    fT[ch, 2 * t + cc] = F2[pl.ds((2 * ch + cc) * XL * TL + t, XL, stride=TL), :]
            return 0

        lax.fori_loop(0, TL // 4, step, 0)
        swap_all(fT, ch)

    low = lax.broadcasted_iota(jnp.int32, (XL, R), 1) < RW

    def swap_halves(ref, ch, yy):
        at = 6 * yy + 2
        one, two = ref[ch, at], ref[ch, at + 1]
        ref[ch, at] = jnp.where(low, one, pltpu.roll(two, RW, axis=1))
        ref[ch, at + 1] = jnp.where(low, pltpu.roll(one, RW, axis=1), two)

    def swap_all(ref, ch):
        def step(group, _):
            for i in range(4):
                swap_halves(ref, ch, 4 * group + i)
            return 0

        lax.fori_loop(0, 2, step, 0)

    def pair_walls():
        load_w.wait()
        for p in range(8):
            WP[p] = jnp.concatenate([W[p], W[p + 8]], axis=1)
        WP2 = WP.reshape(8 * TL, R)
        for t in range(TL):
            wT[t] = WP2[pl.ds(t, 8, stride=TL), :]

    def offset(i):
        return 4 + lax.div(i + 1, 2) * (1 - 2 * lax.rem(i, 2))

    def send(remote, src, dst, s_sem, r_sem, device):
        @pl.when(remote)
        def _():
            pltpu.make_async_remote_copy(
                src_ref=src, dst_ref=dst, send_sem=s_sem, recv_sem=r_sem, device_id=device, device_id_type=MESH
            ).start()

        @pl.when(jnp.logical_not(remote))
        def _():
            pltpu.make_async_copy(src, dst, r_sem).start()

    def theta_peer(i, flip):
        return lax.rem(xh + flip, 2) * 8 + lax.rem(z + offset(i), 8)

    def send_chunk(ch):
        load_f[ch].wait()
        turn(ch)
        if ch == 0:
            pl.semaphore_wait(barrier, NT - 1 + NA - 1)

        def step(i, _):
            for flip in (1, 0):
                t = theta_peer(i, flip)
                send(
                    t != th, F.at[pl.ds(2 * ch, 2), t], Qt.at[pl.ds(2 * ch, 2), pl.ds(TL * th, TL)],
                    sT.at[ch], rT.at[ch], (ax, t, grp),
                )
            yy = lax.rem(y + offset(i), 8)
            for g_to in range(2):
                a_to = 4 * yy + g_to
                send(
                    a_to != a, fT.at[ch, pl.ds(6 * yy + 4 * g_to, 2)], Qx.at[pl.ds(2 * ch, 2), pl.ds(XL * a, XL)],
                    sX.at[ch], rX.at[ch], (2 * yy, th, g_to),
                )
                send(
                    a_to + 2 != a, fT.at[ch, 6 * yy + 2 + g_to], Qx.at[ch, pl.ds(XL * a, XL)],
                    sX.at[ch], rX.at[ch], (2 * yy + 1, th, g_to),
                )
            return 0

        lax.fori_loop(0, 8, step, 0)

    def send_wall():
        def step(i, _):
            p = lax.rem(z + offset(i), 8)
            t = lax.rem(p, 2) * 8 + p
            send(t != th, WP.at[p], Wt.at[pl.ds(TL * th, TL)], sWT, rWT, (ax, t, grp))
            yy = lax.rem(y + offset(i), 8)
            for g_to in range(2):
                slots = pl.ds(0, 2 - g_to)
                send(
                    4 * yy + 2 + g_to != a, wT.at[pl.ds(3 * yy + 2 * g_to, 2 - g_to)], Wx.at[slots, pl.ds(8 * a, 8)],
                    sWX, rWX, (2 * yy + 1, th, g_to),
                )
            return 0

        lax.fori_loop(0, 8, step, 0)

    send_chunk(0)
    pair_walls()
    send_wall()
    send_chunk(1)

    for load in load_rest:
        load.wait()
    lane = lax.broadcasted_iota(jnp.int32, (TL, R), 1)
    m = fm[...]
    row_r = -0.5 * ADVECT_R * m
    row_lift = COUPLE_T * m * m
    wm2 = jnp.concatenate([wm[...], wm[...]], axis=1)
    row_wlift = COUPLE_W * wm2 * wm2

    kk = lax.broadcasted_iota(jnp.int32, (R, R), 0)
    jj = lax.broadcasted_iota(jnp.int32, (R, R), 1)
    spread = 1.0 / m
    spread_t = jnp.broadcast_to(spread, (R, R)).T
    beyond = jnp.sum(jnp.where(kk >= jj, spread_t, 0.0), axis=0, keepdims=True)
    total = jnp.sum(spread_t, axis=0, keepdims=True)
    radius = 1.0 - 0.5 * (beyond - 0.5 * spread) / total
    row_t1 = -ADVECT_T / radius
    row_t2 = 1.0 / (radius * radius)
    wspread = 1.0 / wm2
    wspread_t = jnp.broadcast_to(wspread, (R, R)).T
    within = jnp.sum(jnp.where(kk <= lax.rem(jj, RW), wspread_t, 0.0), axis=0, keepdims=True)
    wtotal = jnp.sum(jnp.where(kk < RW, wspread_t, 0.0), axis=0, keepdims=True)
    wradius = 1.0 + 0.2 * (within - 0.5 * wspread) / wtotal
    row_w2 = LATERAL_W / (wradius * wradius)

    def prepare(p, _):
        pair = WP[p]
        for h in range(2):
            x = p + 8 * h
            u_r = F[2, x] * row_r
            ghost = pltpu.roll(pair, 127 - 64 * h, axis=1)
            for c in range(4):
                q = F[c, x]
                edge = ghost if c == 3 else 0.0
                upper = jnp.where(lane == R - 1, edge, pltpu.roll(q, R - 1, axis=1))
                lower = jnp.where(lane == 0, q, pltpu.roll(q, 1, axis=1))
                value = q + u_r * (upper - lower)
                if c == 3:
                    value = value + jnp.where(lane == R - 1, row_lift * ghost, 0.0)
                base[c, x] = value
        last_0 = pltpu.roll(F[3, p], 1, axis=1)
        last_1 = pltpu.roll(F[3, p + 8], 65, axis=1)
        wbase[p] = pair + jnp.where(
            lane == 0, row_wlift * last_0, jnp.where(lane == RW, row_wlift * last_1, 0.0)
        )
        return 0

    lax.fori_loop(0, 8, prepare, 0)
    for i in range(2):
        parts[i] = inverse_parts(inv[i])

    def full(ref, sem):
        pltpu.make_async_copy(ref, ref, sem).wait()

    half_t = THETA // 2
    half_x = X // 2

    def lam(ch, cc):
        return jnp.where(ch == 1, LATERAL_T, LATERAL_U) if cc == 1 else LATERAL_U

    def theta_chunk(ch):
        both = pl.ds(2 * ch, 2)
        full(Qt.at[both], rT.at[ch])
        top = jnp.concatenate([Qt[2 * ch, :half_t], Qt[2 * ch + 1, :half_t]], axis=1)
        bottom = jnp.concatenate([Qt[2 * ch, half_t:], Qt[2 * ch + 1, half_t:]], axis=1)
        firsts = apply_folded(ttab, slice(0, half_t), top, bottom)
        seconds = apply_folded(ttab, slice(half_t, THETA), top, bottom)
        for h in range(2):
            rows = slice(h * half_t, (h + 1) * half_t)
            swirl = Qt[1, rows] * row_t1
            for cc in range(2):
                cols = slice(cc * R, (cc + 1) * R)
                Rt[2 * ch + cc, rows] = swirl * firsts[h][:, cols] + seconds[h][:, cols] * (row_t2 * lam(ch, cc))

        def step(i, _):
            for flip in (1, 0):
                t = theta_peer(i, flip)
                send(
                    t != th, Rt.at[both, pl.ds(TL * t, TL)], cih.at[both, th], bsT.at[ch], brT.at[ch], (ax, t, grp)
                )
            return 0

        lax.fori_loop(0, 8, step, 0)

    def axial_chunk(ch):
        both = pl.ds(2 * ch, 2)
        full(Qx.at[both], rX.at[ch])
        top = jnp.concatenate([Qx[2 * ch, :half_x], Qx[2 * ch + 1, :half_x]], axis=1)
        bottom = jnp.concatenate([Qx[2 * ch, half_x:], Qx[2 * ch + 1, half_x:]], axis=1)
        firsts = apply_folded(xtab, slice(0, half_x), top, bottom)
        seconds = apply_folded(xtab, slice(half_x, X), top, bottom)
        for h in range(2):
            rows = slice(h * half_x, (h + 1) * half_x)
            stream = Qx[0, rows] * (-ADVECT_X)
            for cc in range(2):
                cols = slice(cc * R, (cc + 1) * R)
                Rx[2 * ch + cc, rows] = stream * firsts[h][:, cols] + seconds[h][:, cols] * lam(ch, cc)

        def step(i, _):
            yy = lax.rem(y + offset(i), 8)
            for k in range(4):
                a_to = 4 * yy + k
                send(
                    a_to != a, Rx.at[both, pl.ds(XL * a_to, XL)], axh.at[ch, pl.ds(2 * my_theta, 2)],
                    bsX.at[ch], brX.at[ch], (2 * yy + k // 2, th, k % 2),
                )
            return 0

        lax.fori_loop(0, 8, step, 0)

    lam_halves = jnp.where(lane[:1] < RW, LATERAL_U, LATERAL_T)

    def axial_half(ch):
        full(Qx.at[ch], rX.at[ch])
        firsts = apply_folded(xtab, slice(0, half_x), Qx[ch, :half_x], Qx[ch, half_x:])
        seconds = apply_folded(xtab, slice(half_x, X), Qx[ch, :half_x], Qx[ch, half_x:])
        lam_row = jnp.where(ch == 1, lam_halves, LATERAL_U)
        low_x = lax.broadcasted_iota(jnp.int32, (half_x, R), 1) < RW
        for h in range(2):
            rows = slice(h * half_x, (h + 1) * half_x)
            stream = Qx[0, rows] * (-ADVECT_X)
            stream = jnp.where(low_x, stream, pltpu.roll(stream, RW, axis=1))
            Rx[ch, rows] = stream * firsts[h] + seconds[h] * lam_row

        def step(i, _):
            yy = lax.rem(y + offset(i), 8)
            for k in range(4):
                a_to = 4 * yy + k
                send(
                    a_to != a, Rx.at[ch, pl.ds(XL * a_to, XL)], axh.at[ch, 6 * y + 2 + grp],
                    bsX.at[ch], brX.at[ch], (2 * yy + k // 2, th, k % 2),
                )
            return 0

        lax.fori_loop(0, 8, step, 0)

    def theta_wall():
        full(Wt, rWT)
        seconds = apply_folded(ttab, slice(half_t, THETA), Wt[:half_t], Wt[half_t:])
        for h in range(2):
            WRt[h * half_t:(h + 1) * half_t] = seconds[h] * row_w2

        def step(i, _):
            for flip in (1, 0):
                t = theta_peer(i, flip)
                send(t != th, WRt.at[pl.ds(TL * t, TL)], cwh.at[z], bsWT, brWT, (ax, t, grp))
            return 0

        lax.fori_loop(0, 8, step, 0)

    low8 = lax.broadcasted_iota(jnp.int32, (8, R), 1) < RW

    def axial_wall(g):
        slots = pl.ds(0, 2 - g)
        full(Wx.at[slots], rWX)

        def unpack(s, _):
            rows = pl.ds(pl.multiple_of(8 * s, 8), 8)
            even = pl.ds(pl.multiple_of(16 * s, 8), 8)
            odd = pl.ds(pl.multiple_of(16 * s + 8, 8), 8)
            w0 = Wx[0, rows]
            w1 = Wx[1 - g, rows]
            Wn[even] = jnp.where(low8, w0, pltpu.roll(w1, RW, axis=1))
            Wn[odd] = jnp.where(low8, pltpu.roll(w0, RW, axis=1), w1)
            return 0

        lax.fori_loop(0, NA, unpack, 0)
        seconds = apply_folded(xtab, slice(half_x, X), Wn[:half_x], Wn[half_x:])
        for h in range(2):
            Wn[h * half_x:(h + 1) * half_x] = seconds[h] * LATERAL_W

        def pack(s, _):
            rows = pl.ds(pl.multiple_of(8 * s, 8), 8)
            even = Wn[pl.ds(pl.multiple_of(16 * s, 8), 8)]
            odd = Wn[pl.ds(pl.multiple_of(16 * s + 8, 8), 8)]
            WRx[0, rows] = jnp.where(low8, even, pltpu.roll(odd, RW, axis=1))
            if g == 0:
                WRx[1, rows] = jnp.where(low8, pltpu.roll(even, RW, axis=1), odd)
            return 0

        lax.fori_loop(0, NA, pack, 0)

        def step(i, _):
            yy = lax.rem(y + offset(i), 8)
            for k in range(4):
                a_to = 4 * yy + k
                send(
                    a_to != a, WRx.at[slots, pl.ds(8 * a_to, 8)], awh.at[pl.ds(3 * y + 2 * g, 2 - g)],
                    bsWX, brWX, (2 * yy + k // 2, th, k % 2),
                )
            return 0

        lax.fori_loop(0, 8, step, 0)

    theta_chunk(0)
    pl.when(x_whole)(lambda: axial_chunk(0))
    pl.when(x_half)(lambda: axial_half(0))
    pl.when(jnp.logical_and(x_half, grp == 0))(lambda: axial_wall(0))
    pl.when(jnp.logical_and(x_half, grp == 1))(lambda: axial_wall(1))
    pl.when(t_wall)(theta_wall)
    theta_chunk(1)
    pl.when(x_whole)(lambda: axial_chunk(1))
    pl.when(x_half)(lambda: axial_half(1))

    axh2 = axh.reshape(4 * XL * TL, R)

    def gather(ch, out):
        full(cih.at[pl.ds(2 * ch, 2)], brT.at[ch])

        def add_circle(group, _):
            for i in range(4):
                for cc in range(2):
                    out[cc, 4 * group + i] = base[2 * ch + cc, 4 * group + i] + cih[2 * ch + cc, 4 * group + i]
            return 0

        lax.fori_loop(0, XL // 4, add_circle, 0)
        full(axh.at[ch], brX.at[ch])
        swap_all(axh, ch)

        def add(group, _):
            for i in range(4):
                x = 4 * group + i
                for cc in range(2):
                    axial = axh2[pl.ds(ch * 2 * XL * TL + cc * XL + x, TL, stride=2 * XL), :]
                    out[cc, x] = out[cc, x] + axial
            return 0

        lax.fori_loop(0, XL // 4, add, 0)

    gather(0, done)
    for c in range(2):
        done[c] = apply_inverse(parts[0], done[c].reshape(XL * TL, R)).reshape(XL, TL, R)
    full(cwh, brWT)
    full(awh, brWX)
    awh2 = awh.reshape(8 * TL, R)

    def gather_wall(p, _):
        wbase[p] = wbase[p] + cwh[p] + awh2[pl.ds(p, TL, stride=8), :]
        return 0

    lax.fori_loop(0, 8, gather_wall, 0)
    value = wbase[...].reshape(8 * TL, R)
    nothing = jnp.zeros((RW, RW), F32)
    for h in range(2):
        pair = [winv[...], nothing] if h == 0 else [nothing, winv[...]]
        matrix = inverse_parts(jnp.concatenate(pair, axis=1))
        wdone[8 * h:8 * h + 8] = apply_inverse(matrix, value).reshape(8, TL, RW)
    gather(1, rest)

    for ch in range(2):
        full(F.at[pl.ds(0, 2), pl.ds(0, NT - 1)], sT.at[ch])
        full(F.at[pl.ds(0, 2), pl.ds(0, NT - 1)], bsT.at[ch])

        @pl.when(x_whole)
        def _():
            full(fT.at[ch, pl.ds(0, 2 * TL - 2)], sX.at[ch])
            full(Rx.at[pl.ds(0, 2), pl.ds(0, X - XL)], bsX.at[ch])

        @pl.when(x_half)
        def _():
            full(fT.at[ch, pl.ds(0, 2 * TL - 1)], sX.at[ch])
            full(Rx.at[0, pl.ds(0, X - XL)], bsX.at[ch])

    @pl.when(t_wall)
    def _():
        full(WP.at[pl.ds(0, 7)], sWT)
        full(WRt.at[pl.ds(0, THETA - TL)], bsWT)

    @pl.when(jnp.logical_not(t_wall))
    def _():
        full(WP, sWT)

    @pl.when(x_whole)
    def _():
        full(wT, sWX)

    for g in range(2):
        @pl.when(jnp.logical_and(x_half, grp == g))
        def _():
            full(wT.at[pl.ds(0, TL - 2 + g)], sWX)
            full(WRx.at[pl.ds(0, 2 - g), pl.ds(0, 8 * (NA - 1))], bsWX)


def last_kernel(done, rest, wdone, parts, out_h, wout_h, buf, st):
    copies = [
        pltpu.make_async_copy(done, out_h.at[pl.ds(0, 2)], st.at[0]),
        pltpu.make_async_copy(wdone, wout_h, st.at[1]),
    ]
    for copy in copies:
        copy.start()
    for c in range(2):
        for h in range(2):
            rows = slice(h * XL // 2, (h + 1) * XL // 2)
            value = rest[c, rows].reshape(XL * TL // 2, R)
            buf[c, rows] = apply_inverse(parts[c], value).reshape(XL // 2, TL, R)
            some = pl.ds(h * XL // 2, XL // 2)
            copy = pltpu.make_async_copy(buf.at[c, some], out_h.at[2 + c, some], st.at[2 + 2 * c + h])
            copy.start()
            copies.append(copy)
    for copy in copies:
        copy.wait()


def shards(fields, wall_temp, fluid_metric, fluid_radial_inverses, wall_metric, wall_inverse):
    vmem = pl.BlockSpec(memory_space=pltpu.VMEM)
    hbm = pl.BlockSpec(memory_space=pltpu.HBM)
    dma = pltpu.SemaphoreType.DMA
    ttab = jnp.asarray(folded_tables(THETA))
    xtab = jnp.asarray(folded_tables(X))

    def buf(*shape, dtype=F32):
        return pltpu.VMEM(shape, dtype)

    done, rest, wdone, parts = pl.pallas_call(
        kernel,
        out_shape=(buf(2, XL, TL, R), buf(2, XL, TL, R), buf(XL, TL, RW), buf(2, R, 3 * R, dtype=BF16)),
        in_specs=[hbm] * 8,
        out_specs=(vmem,) * 4,
        scratch_shapes=[
            buf(4, XL, TL, R), buf(XL, TL, RW), buf(1, R), buf(2, R, R), buf(1, RW), buf(RW, RW),
            buf(*ttab.shape, dtype=BF16), buf(*xtab.shape, dtype=BF16),
            buf(2, 2 * TL, XL, R), buf(8, TL, R), buf(TL, 8, R),
            buf(4, THETA, R), buf(4, X, R), buf(THETA, R), buf(2, X // 2, R),
            buf(4, THETA, R), buf(4, X, R), buf(THETA, R), buf(2, X // 2, R), buf(X, R),
            buf(4, XL, TL, R), buf(2, 2 * TL, XL, R), buf(8, TL, R), buf(TL, 8, R),
            buf(4, XL, TL, R), buf(8, TL, R),
            dma((9,)),
            dma((2,)), dma((2,)), dma((2,)), dma((2,)), dma, dma, dma, dma,
            dma((2,)), dma((2,)), dma((2,)), dma((2,)), dma, dma, dma, dma,
        ],
        compiler_params=pltpu.CompilerParams(
            collective_id=0, has_side_effects=True, vmem_limit_bytes=64128 * 2**10
        ),
    )(
        fields, wall_temp, fluid_metric.reshape(1, R), fluid_radial_inverses,
        wall_metric.reshape(1, RW), wall_inverse, ttab, xtab,
    )
    return pl.pallas_call(
        last_kernel,
        out_shape=(
            jax.ShapeDtypeStruct((4, XL, TL, R), F32),
            jax.ShapeDtypeStruct((XL, TL, RW), F32),
        ),
        in_specs=[vmem] * 4,
        out_specs=(hbm, hbm),
        scratch_shapes=[buf(2, XL, TL, R), dma((6,))],
        compiler_params=pltpu.CompilerParams(vmem_limit_bytes=16 * 2**20),
    )(done, rest, wdone, parts)


def solution(mesh):
    in_specs = (
        P(None, ("ax", "grp"), "th", None),
        P(("ax", "grp"), "th", None),
        P(),
        P(),
        P(),
        P(),
    )
    out_specs = (P(None, ("ax", "grp"), "th", None), P(("ax", "grp"), "th", None))
    return jax.shard_map(shards, mesh=mesh, in_specs=in_specs, out_specs=out_specs, check_vma=False)
```
